32 devices in a mesh: band: 8 (over z, x), sector: 4 (over y, core).
Axes of the slice: x: 2, y: 2, z: 4, core: 2. Of those that a mesh axis runs over, the one named last changes fastest.
Arguments:
- node_latent: bfloat16 [16384, 256], P(('band', 'sector')), may hold values from -6 to 6
- edge_latent: bfloat16 [196608, 256], P(('band', 'sector')), may hold values from -6 to 6
- sender_slot: int32 [16384, 12], P(('band', 'sector')), may hold values from 0 to 1023, as said below
- edge_mask: int32 [16384, 12], P(('band', 'sector')), may hold values 0 or 1
- send_rows: int32 [32, 8, 64], P(('band', 'sector')), may hold values from 0 to 511
- w_edge_in: bfloat16 [768, 256], replicated, may hold values from -0.21875 to 0.21875
- b_edge: float32 [256], replicated, may hold values from -3 to 3
- w_edge_out: bfloat16 [256, 256], replicated, may hold values from -0.375 to 0.375
- g_edge: float32 [256], replicated, may hold values from 0.1 to 1.9
- w_node_in: bfloat16 [512, 256], replicated, may hold values from -0.25 to 0.25
- b_node: float32 [256], replicated, may hold values from -3 to 3
- w_node_out: bfloat16 [256, 256], replicated, may hold values from -0.375 to 0.375
- g_node: float32 [256], replicated, may hold values from 0.1 to 1.9
- node_cot: bfloat16 [16384, 256], P(('band', 'sector')), may hold values from -6 to 6
- edge_cot: bfloat16 [196608, 256], P(('band', 'sector')), may hold values from -6 to 6
Outputs:
- node_new: bfloat16 [16384, 256], P(('band', 'sector'))
- edge_new: bfloat16 [196608, 256], P(('band', 'sector'))
- node_grad: float32 [16384, 256], P(('band', 'sector'))
- edge_grad: bfloat16 [196608, 256], P(('band', 'sector'))
- grad_edge_in: float32 [768, 256], replicated
- grad_edge_out: float32 [256, 256], replicated
- grad_node_in: float32 [512, 256], replicated
- grad_node_out: float32 [256, 256], replicated
The draws below stay inside these ranges and needn't reach their ends.
Inputs may be any that keep to these rules, and one draw needn't show every extreme that they name: `sender_slot`: values below 512 name the receiver owner's own nodes; value 512 + j * 64 + c names row send_rows[q, j, c] of the neighbouring owner q in direction j; directions that would leave the first or last band never occur.
All inputs are finite; a program needn't handle non-finite values. No bound on the sum of `edge_mask` on one device may be relied on, other than what follows from the above.
Results may differ from the reference program's by a relative error of at most 0.013.
Values may be sent and summed in bfloat16 or wider, within the bound.
No kernel may reach another device: no remote copies, remote signals or barrier semaphores. Data moves between devices by JAX's collectives and lax.ppermute only.
A program may use at most 128 MiB of HBM per device.

```python
import jax
import jax.numpy as jnp
from jax import lax

D = 256
NODE_DEV = 512
K = 12
CAP = 64
NODES = 16384
EDGES = 196608
N_BAND = 8
N_SECTOR = 4


band_steps = (-1, -1, -1, 0, 0, 1, 1, 1)


def draw_sender_slot(key, part):
    first_key = jax.random.fold_in(key, 11)
    second_key = jax.random.fold_in(key, 12)
    third_key = jax.random.fold_in(key, 13)
    course = jax.random.randint(first_key, (NODES, K), 0, 9)
    column = jax.random.randint(second_key, (NODES, K), 0, CAP)
    local_row = jax.random.randint(third_key, (NODES, K), 0, NODE_DEV)
    owner = jnp.arange(NODES, dtype=jnp.int32) // NODE_DEV
    own_band = (owner // N_SECTOR)[:, None]
    band_table = jnp.array(band_steps + (0,), dtype=jnp.int32)
    far_band = own_band + band_table[course]
    valid = (course < 8) & (far_band >= 0) & (far_band < N_BAND)
    values = jnp.where(valid, NODE_DEV + course * CAP + column, local_row)
    leading = (jnp.arange(NODES, dtype=jnp.int32) % NODE_DEV == 0)[:, None]
    slot_index = jnp.arange(K, dtype=jnp.int32)[None, :]
    highest = jnp.where(own_band < N_BAND - 1, NODE_DEV + 8 * CAP - 1, NODE_DEV + 5 * CAP - 1)
    values = jnp.where(leading & (slot_index == 0), highest, values)
    values = jnp.where(leading & (slot_index == 1), 0, values)
    return values.astype(jnp.int32)


def touch_ends(drawn, own_key, least, top_value):
    index_at = [jax.random.randint(jax.random.fold_in(own_key, axis), (), 0, length) for axis, length in enumerate(drawn.shape)]
    widest = drawn.shape.index(max(drawn.shape))
    beside = index_at[:widest] + [(index_at[widest] + 1) % drawn.shape[widest]] + index_at[widest + 1:]
    return drawn.at[tuple(index_at)].set(least).at[tuple(beside)].set(top_value)


def level_of(key, extent, split, least, largest):
    factor_of, own = 1.0, jax.random.fold_in(key, 6)
    for axis_at, parts in split:
        steps = jnp.exp(jax.random.uniform(jax.random.fold_in(own, axis_at), (parts,), jnp.float32, least / len(split), largest / len(split)))
        factor_of = factor_of * jnp.repeat(steps, extent[axis_at] // parts).reshape([-1 if axis == axis_at else 1 for axis in range(len(extent))])
    return factor_of


def gaussian(key, extent, spread, limit, shards=(), kind=jnp.bfloat16):
    values = jax.random.normal(key, extent, jnp.float32) * spread
    if len(shards) > 0:
        values = level_of(key, extent, shards, -0.22, 0.18) * values
    return jnp.clip(values, min=-limit, max=limit).astype(kind)


def setup_inputs(seed: int = 0) -> dict:
    streams_of = jax.random.split(jax.random.key(seed), 16)
    return {
        "node_latent": gaussian(streams_of[0], (NODES, D), 1.0, 6.0, ((0, 32),)),
        "edge_latent": gaussian(streams_of[1], (EDGES, D), 1.0, 6.0, ((0, 32),)),
        "sender_slot": draw_sender_slot(jax.random.fold_in(streams_of[15], 71), 0),
        "edge_mask": touch_ends((jax.random.randint(streams_of[3], (NODES, K), 0, 3) < 2).astype(jnp.int32), jax.random.fold_in(streams_of[3], 1), 0, 1),
        "send_rows": touch_ends(jax.random.randint(streams_of[4], (N_BAND * N_SECTOR, 8, CAP), 0, NODE_DEV), jax.random.fold_in(streams_of[4], 1), 0, NODE_DEV - 1).astype(jnp.int32),
        "w_edge_in": gaussian(streams_of[5], (3 * D, D), (3 * D) ** -0.5, 0.21875),
        "b_edge": gaussian(streams_of[6], (D,), 0.5, 3.0, (), jnp.float32),
        "w_edge_out": gaussian(streams_of[7], (D, D), D ** -0.5, 0.375),
        "g_edge": jnp.clip(1.0 + 0.18 * jax.random.normal(streams_of[8], (D,), jnp.float32), 0.1, 1.9),
        "w_node_in": gaussian(streams_of[9], (2 * D, D), (2 * D) ** -0.5, 0.25),
        "b_node": gaussian(streams_of[10], (D,), 0.5, 3.0, (), jnp.float32),
        "w_node_out": gaussian(streams_of[11], (D, D), D ** -0.5, 0.375),
        "g_node": jnp.clip(1.0 + 0.18 * jax.random.normal(streams_of[12], (D,), jnp.float32), 0.1, 1.9),
        "node_cot": gaussian(streams_of[13], (NODES, D), 1.0, 6.0, ((0, 32),)),
        "edge_cot": gaussian(streams_of[14], (EDGES, D), 1.0, 6.0, ((0, 32),)),
    }


band_steps = (-1, -1, -1, 0, 0, 1, 1, 1)
sector_steps = (-1, 0, 1, -1, 1, -1, 0, 1)

def layer_norm(values, gain):
    average = lax.optimization_barrier(jnp.mean(values, -1, keepdims=True))
    centred = values - average
    variance = lax.optimization_barrier(jnp.mean(centred * centred, -1, keepdims=True))
    return centred * lax.rsqrt(variance + 1e-05) * gain

def interact(own_f, sender_f, edge_block, mask_f, w_edge_in, b_edge, w_edge_out, g_edge, w_node_in, b_node, w_node_out, g_node):
    latent_width = own_f.shape[1]
    node_count = own_f.shape[0]
    slot_count = sender_f.shape[0] // node_count
    own_rows = own_f.astype(jnp.bfloat16)
    sender = sender_f.astype(jnp.bfloat16)
    from_edge = jnp.dot(edge_block, w_edge_in[:latent_width], preferred_element_type=jnp.float32)
    from_sender = jnp.dot(sender, w_edge_in[latent_width:2 * latent_width], preferred_element_type=jnp.float32)
    from_receiver = jnp.dot(own_rows, w_edge_in[2 * latent_width:], preferred_element_type=jnp.float32)
    pre_edge = (from_edge + from_sender).reshape(node_count, slot_count, latent_width) + from_receiver[:, None, :] + b_edge
    hidden = jax.nn.silu(pre_edge).astype(jnp.bfloat16).reshape(node_count * slot_count, latent_width)
    update = layer_norm(jnp.dot(hidden, w_edge_out, preferred_element_type=jnp.float32), g_edge) * mask_f
    edge_new = (edge_block.astype(jnp.float32) + update).astype(jnp.bfloat16)
    gathered = update.reshape(node_count, slot_count, latent_width).sum(1).astype(jnp.bfloat16)
    pre_node = jnp.dot(own_rows, w_node_in[:latent_width], preferred_element_type=jnp.float32)
    pre_node = pre_node + jnp.dot(gathered, w_node_in[latent_width:], preferred_element_type=jnp.float32) + b_node
    hidden_node = jax.nn.silu(pre_node).astype(jnp.bfloat16)
    node_new = (own_f + layer_norm(jnp.dot(hidden_node, w_node_out, preferred_element_type=jnp.float32), g_node)).astype(jnp.bfloat16)
    return (node_new, edge_new)

def differentiate(own_f, sender_f, edge_block, mask_f, weights, node_cot, edge_cot):
    w_edge_in, b_edge, w_edge_out, g_edge, w_node_in, b_node, w_node_out, g_node = weights

    def local_layer(own_in, sender_in, edge_in, first_edge, second_edge, first_node, second_node):
        return interact(own_in, sender_in, edge_in, mask_f, first_edge, b_edge, second_edge, g_edge, first_node, b_node, second_node, g_node)
    results, pullback = jax.vjp(local_layer, own_f, sender_f, edge_block, w_edge_in, w_edge_out, w_node_in, w_node_out)
    return (results, pullback((node_cot, edge_cot)))

def reference(node_latent, edge_latent, sender_slot, edge_mask, send_rows, w_edge_in, b_edge, w_edge_out, g_edge, w_node_in, b_node, w_node_out, g_node, node_cot, edge_cot):
    node_count = NODE_DEV
    peer_count = N_BAND * N_SECTOR
    latent_width = D
    slot_count = K
    weights = (w_edge_in, b_edge, w_edge_out, g_edge, w_node_in, b_node, w_node_out, g_node)
    node_f = node_latent.astype(jnp.float32)
    band_table = jnp.array(band_steps, dtype=jnp.int32)
    sector_table = jnp.array(sector_steps, dtype=jnp.int32)

    def per_block(carried, block_data):
        node_total, weight_totals = carried
        owner_index, edge_block, slot_block, mask_block, node_part, edge_part = block_data
        first_row = owner_index * node_count
        own_band = owner_index // N_SECTOR
        own_sector = owner_index % N_SECTOR
        own_f = lax.dynamic_slice_in_dim(node_f, first_row, node_count, 0)
        slot_flat = slot_block.reshape(-1)
        remote = jnp.maximum(slot_flat - node_count, 0)
        course = jnp.minimum(remote // CAP, 7)
        column = remote % CAP
        far_band = jnp.clip(own_band + band_table[course], 0, N_BAND - 1)
        far_sector = (own_sector + sector_table[course]) % N_SECTOR
        neighbour = (far_band * N_SECTOR + far_sector).astype(jnp.int32)
        far_row = send_rows[neighbour, course, column]
        global_index = jnp.where(slot_flat < node_count, first_row + slot_flat, neighbour * node_count + far_row).astype(jnp.int32)
        sender_f = node_f[global_index]
        mask_f = mask_block.reshape(-1, 1).astype(jnp.float32)
        results, gradients = differentiate(own_f, sender_f, edge_block, mask_f, weights, node_part, edge_part)
        d_own, d_sender, d_edge, g_first, g_second, g_third, g_fourth = gradients
        node_total = node_total.at[global_index].add(d_sender)
        current = lax.dynamic_slice_in_dim(node_total, first_row, node_count, 0)
        node_total = lax.dynamic_update_slice_in_dim(node_total, current + d_own, first_row, 0)
        weight_totals = tuple((total + part.astype(jnp.float32) for total, part in zip(weight_totals, (g_first, g_second, g_third, g_fourth))))
        return ((node_total, weight_totals), (results[0], results[1], d_edge))
    block_inputs = (jnp.arange(peer_count, dtype=jnp.int32), edge_latent.reshape(peer_count, node_count * slot_count, latent_width), sender_slot.reshape(peer_count, node_count, slot_count), edge_mask.reshape(peer_count, node_count, slot_count), node_cot.reshape(peer_count, node_count, latent_width), edge_cot.reshape(peer_count, node_count * slot_count, latent_width))
    initial = (jnp.zeros((peer_count * node_count, latent_width), jnp.float32), tuple((jnp.zeros(matrix.shape, jnp.float32) for matrix in (w_edge_in, w_edge_out, w_node_in, w_node_out))))
    (node_grad, weight_totals), (node_new, edge_new, edge_grad) = lax.scan(per_block, initial, block_inputs)
    grad_scale = float(peer_count * node_count * slot_count) ** (-0.5)
    return (node_new.reshape(-1, latent_width), edge_new.reshape(-1, latent_width), node_grad, edge_grad.reshape(-1, latent_width), weight_totals[0] * grad_scale, weight_totals[1] * grad_scale, weight_totals[2] * grad_scale, weight_totals[3] * grad_scale)
```

```python
import functools

import jax
import jax.numpy as jnp
from jax import lax
from jax.experimental import pallas as pl
from jax.experimental.pallas import tpu as pltpu
from jax.sharding import PartitionSpec as P

band_steps = (-1, -1, -1, 0, 0, 1, 1, 1)
sector_steps = (-1, 0, 1, -1, 1, -1, 0, 1)
BF16 = jnp.bfloat16
F32 = jnp.float32


def passed_along(array, axis, by):
    count = lax.axis_size(axis)
    return lax.ppermute(array, axis, [(i, (i + by) % count) for i in range(count)])


def from_behind(array, axis, by):
    count = lax.axis_size(axis)
    pairs = [(i, i + by) for i in range(count) if 0 <= i + by < count]
    return lax.ppermute(array, axis, pairs)


def exchange(pieces, order):
    held = list(pieces)
    for axis, back in order:
        steps = sector_steps if axis == "sector" else band_steps
        move = passed_along if axis == "sector" else from_behind
        moved = []
        for heading in (1, -1):
            members = [course for course in range(8) if steps[course] == heading]
            sent = jnp.concatenate([held[course] for course in members])
            moved.append((members, move(sent, axis, heading if back else -heading)))
        for members, block in moved:
            rows = block.shape[0] // len(members)
            for place, course in enumerate(members):
                held[course] = block[place * rows : (place + 1) * rows]
    return held


def swapped(array, axis, mask):
    count = lax.axis_size(axis)
    return lax.ppermute(array, axis, [(i, i ^ mask) for i in range(count)])


def summed_over_devices(array):
    rounds = []
    for axis in ("sector", "band"):
        step = 1
        while step < lax.axis_size(axis):
            rounds.append((axis, step))
            step *= 2
    held = array
    bits = []
    for axis, step in rounds:
        bit = (lax.axis_index(axis) // step) % 2
        half = held.shape[0] // 2
        keep = lax.dynamic_slice_in_dim(held, bit * half, half, 0)
        give = lax.dynamic_slice_in_dim(held, (1 - bit) * half, half, 0)
        got = swapped(give, axis, step)
        held = (keep.astype(F32) + got.astype(F32)).astype(BF16)
        bits.append(bit)
    for (axis, step), bit in reversed(list(zip(rounds, bits))):
        got = swapped(held, axis, step)
        held = jnp.concatenate(
            [jnp.where(bit == 0, held, got), jnp.where(bit == 0, got, held)], axis=0
        )
    return held


def dot(a, b, ca=1, cb=0):
    return lax.dot_general(a, b, (((ca,), (cb,)), ((), ())), preferred_element_type=F32)


def row_mean(values):
    return jnp.mean(values, axis=-1, keepdims=True)


def silu_parts(v):
    gate = 0.5 * jnp.tanh(0.5 * v) + 0.5
    out = v * gate
    return out, gate + out * (1.0 - gate)


def provide_kernel(rows_ref, node_ref, out_ref):
    count = node_ref.shape[0]
    lanes = lax.broadcasted_iota(jnp.int32, (rows_ref.shape[0], count), 1)
    pick = jnp.where(rows_ref[...] == lanes, 1.0, 0.0).astype(BF16)
    out_ref[...] = dot(pick, node_ref[...]).astype(BF16)


def collect_kernel(rows_ref, arrived_ref, partial_ref, w_ref, out_ref):
    count = partial_ref.shape[0]
    lines = lax.broadcasted_iota(jnp.int32, (count, rows_ref.shape[1]), 0)
    pick = jnp.where(rows_ref[...] == lines, 1.0, 0.0).astype(BF16)
    total = dot(pick, arrived_ref[...]).astype(BF16)
    out_ref[...] = partial_ref[...] + dot(total, w_ref[...], 1, 1)


def layer_kernel(
    own_ref,
    far_ref,
    slot_ref,
    mask_ref,
    slot_row_ref,
    w_in_ref,
    b_edge_ref,
    w_out_ref,
    g_edge_ref,
    wn_in_ref,
    b_node_ref,
    wn_out_ref,
    g_node_ref,
    node_cot_ref,
    edge_hbm,
    cot_hbm,
    node_new_ref,
    new_hbm,
    partial_ref,
    grad_hbm,
    back_ref,
    wg_ref,
    edge_v,
    cot_v,
    new_v,
    grad_v,
    hid_v,
    slope_v,
    norm_v,
    scale_v,
    code_v,
    table_v,
    proj_v,
    recv_v,
    gath_v,
    dgath_v,
    drecv_v,
    wide_v,
    t_acc,
    we_acc,
    wo_acc,
    sem_in,
    sem_out,
    *,
    chunk,
):
    d = own_ref.shape[1]
    nodes = own_ref.shape[0]
    edges = edge_v.shape[0]
    slots = edges // nodes
    table = nodes + far_ref.shape[0]
    count = edges // chunk
    cn = chunk // slots

    def piece(index):
        return pl.ds(pl.multiple_of(index * chunk, chunk), chunk)

    def pull(kind, index):
        src, dst = ((edge_hbm, edge_v), (cot_hbm, cot_v))[kind]
        return pltpu.make_async_copy(src.at[piece(index)], dst.at[piece(index)], sem_in.at[kind, index])

    def push(kind, index):
        src, dst = ((new_v, new_hbm), (grad_v, grad_hbm))[kind]
        return pltpu.make_async_copy(src.at[piece(index)], dst.at[piece(index)], sem_out.at[kind, index])

    for kind in range(2):
        for index in range(count):
            pull(kind, index).start()

    code = slot_ref[...] * 2 + mask_ref[...]
    for k in range(slots):
        code_v[pl.ds(k, nodes, stride=slots), :] = jnp.broadcast_to(code[:, k : k + 1], (nodes, 128))

    own = own_ref[...]
    table_v[:nodes, :] = own
    table_v[nodes:, :] = far_ref[...]
    proj_v[...] = dot(table_v[...], w_in_ref[d : 2 * d, :]).astype(BF16)
    recv_v[...] = dot(own, w_in_ref[2 * d :, :]) + b_edge_ref[...]
    gain = g_edge_ref[...]
    lanes = lax.broadcasted_iota(jnp.int32, (chunk, 128), 1)

    def spread(source, index):
        rows = source[pl.ds(pl.multiple_of(index * cn, cn), cn), :]
        for k in range(slots):
            for lo in (0, 128):
                wide_v[lo // 128, pl.ds(k, cn, stride=slots), :] = rows[:, lo : lo + 128]

    def wide():
        return jnp.concatenate([wide_v[0], wide_v[1]], axis=1)

    def put_wide(values):
        wide_v[0] = values[:, :128]
        wide_v[1] = values[:, 128:]

    def folded():
        parts = []
        for half in range(2):
            total = wide_v[half, pl.ds(0, cn, stride=slots), :]
            for k in range(1, slots):
                total = total + wide_v[half, pl.ds(k, cn, stride=slots), :]
            parts.append(total)
        return jnp.concatenate(parts, axis=1)

    def ahead(index, carry):
        rows = piece(index)
        pull(0, index).wait()
        edge = edge_v[rows, :]
        spread(recv_v, index)
        code = code_v[rows, :]
        slot = lax.shift_right_logical(code, 1)
        pick = jnp.concatenate(
            [jnp.where(slot == lanes + at, 1.0, 0.0).astype(BF16) for at in range(0, table, 128)], axis=1
        )
        pre = dot(edge, w_in_ref[:d, :]) + dot(pick, proj_v[...]) + wide()
        hidden, slope = silu_parts(pre)
        hidden = hidden.astype(BF16)
        hid_v[rows, :] = hidden
        slope_v[rows, :] = slope.astype(BF16)
        y = dot(hidden, w_out_ref[...])
        y = y - row_mean(y)
        rstd = lax.rsqrt(row_mean(y * y) + 1e-05)
        norm = y * rstd
        norm_v[rows, :] = norm.astype(BF16)
        valid = (code & 1).astype(F32)
        scale_v[rows, :] = valid * rstd
        update = norm * valid[:, :1] * gain
        new_v[rows, :] = (edge.astype(F32) + update).astype(BF16)
        put_wide(update)
        gath_v[pl.ds(pl.multiple_of(index * cn, cn), cn), :] = folded().astype(BF16)
        push(0, index).start()
        return carry

    lax.fori_loop(0, count, ahead, 0)

    gathered = gath_v[...]
    pre = dot(own, wn_in_ref[:d, :]) + dot(gathered, wn_in_ref[d:, :]) + b_node_ref[...]
    hidden, slope = silu_parts(pre)
    hidden = hidden.astype(BF16)
    y = dot(hidden, wn_out_ref[...])
    y = y - row_mean(y)
    rstd = lax.rsqrt(row_mean(y * y) + 1e-05)
    norm = y * rstd
    node_new_ref[...] = (own.astype(F32) + norm * g_node_ref[...]).astype(BF16)
    node_cot = node_cot_ref[...].astype(F32)
    a = node_cot * g_node_ref[...]
    dy = ((a - row_mean(a) - norm * row_mean(a * norm)) * rstd).astype(BF16)
    dpre = (dot(dy, wn_out_ref[...], 1, 1) * slope).astype(BF16)
    dgath_v[...] = dot(dpre, wn_in_ref[d:, :], 1, 1)
    partial_ref[...] = node_cot + dot(dpre, wn_in_ref[:d, :], 1, 1)
    wg_ref[4 * d : 5 * d, :] = dot(own, dpre, 0, 0).astype(BF16)
    wg_ref[5 * d : 6 * d, :] = dot(gathered, dpre, 0, 0).astype(BF16)
    wg_ref[6 * d : 7 * d, :] = dot(hidden, dy, 0, 0).astype(BF16)

    t_acc[...] = jnp.zeros_like(t_acc)
    we_acc[...] = jnp.zeros_like(we_acc)
    wo_acc[...] = jnp.zeros_like(wo_acc)
    lines = lax.broadcasted_iota(jnp.int32, (table, chunk), 0)

    def behind(index, carry):
        rows = piece(index)
        pull(1, index).wait()
        cot = cot_v[rows, :].astype(F32)
        spread(dgath_v, index)
        a = (cot + wide()) * gain
        norm = norm_v[rows, :].astype(F32)
        dy = ((a - row_mean(a) - norm * row_mean(a * norm)) * scale_v[rows, :][:, :1]).astype(BF16)
        dpre = dot(dy, w_out_ref[...], 1, 1) * slope_v[rows, :].astype(F32)
        put_wide(dpre)
        drecv_v[pl.ds(pl.multiple_of(index * cn, cn), cn), :] = folded().astype(BF16)
        dpre = dpre.astype(BF16)
        grad_v[rows, :] = (cot + dot(dpre, w_in_ref[:d, :], 1, 1)).astype(BF16)
        push(1, index).start()
        wo_acc[...] += dot(hid_v[rows, :], dy, 0, 0)
        we_acc[...] += dot(edge_v[rows, :], dpre, 0, 0)
        pick = jnp.where(slot_row_ref[:, rows] == lines, 1.0, 0.0).astype(BF16)
        t_acc[...] += dot(pick, dpre)
        return carry

    lax.fori_loop(0, count, behind, 0)

    total = t_acc[...].astype(BF16)
    back_ref[...] = total[nodes:, :]
    drecv = drecv_v[...]
    partial_ref[...] += dot(total[:nodes, :], w_in_ref[d : 2 * d, :], 1, 1) + dot(drecv, w_in_ref[2 * d :, :], 1, 1)
    wg_ref[:d, :] = we_acc[...].astype(BF16)
    wg_ref[d : 2 * d, :] = dot(table_v[...], total, 0, 0).astype(BF16)
    wg_ref[2 * d : 3 * d, :] = dot(own, drecv, 0, 0).astype(BF16)
    wg_ref[3 * d : 4 * d, :] = wo_acc[...].astype(BF16)
    for kind in range(2):
        for index in range(count):
            push(kind, index).wait()


def local(
    node_latent,
    edge_latent,
    sender_slot,
    edge_mask,
    send_rows,
    w_edge_in,
    b_edge,
    w_edge_out,
    g_edge,
    w_node_in,
    b_node,
    w_node_out,
    g_node,
    node_cot,
    edge_cot,
):
    nodes, d = node_latent.shape
    edges = edge_latent.shape[0]
    slots = sender_slot.shape[1]
    capacity = send_rows.shape[2]
    far = 8 * capacity
    table = nodes + far
    devices = lax.axis_size("band") * lax.axis_size("sector")
    params = pltpu.CompilerParams(vmem_limit_bytes=60000 * 1024)
    shape = jax.ShapeDtypeStruct
    outgoing = pl.pallas_call(
        provide_kernel, out_shape=shape((far, d), BF16), compiler_params=params
    )(send_rows.reshape(far, 1), node_latent)
    pieces = [outgoing[j * capacity : (j + 1) * capacity] for j in range(8)]
    received = jnp.concatenate(exchange(pieces, (("sector", False), ("band", False))))

    chunk = 64 * slots
    vmem = pl.BlockSpec(memory_space=pltpu.VMEM)
    hbm = pl.BlockSpec(memory_space=pl.ANY)
    node_new, edge_new, partial, edge_grad, back, grads = pl.pallas_call(
        functools.partial(layer_kernel, chunk=chunk),
        out_shape=(
            shape((nodes, d), BF16),
            shape((edges, d), BF16),
            shape((nodes, d), F32),
            shape((edges, d), BF16),
            shape((far, d), BF16),
            shape((7 * d, d), BF16),
        ),
        in_specs=[vmem] * 14 + [hbm] * 2,
        out_specs=(vmem, hbm, vmem, hbm, vmem, vmem),
        scratch_shapes=[
            pltpu.VMEM((edges, d), BF16),
            pltpu.VMEM((edges, d), BF16),
            pltpu.VMEM((edges, d), BF16),
            pltpu.VMEM((edges, d), BF16),
            pltpu.VMEM((edges, d), BF16),
            pltpu.VMEM((edges, d), BF16),
            pltpu.VMEM((edges, d), BF16),
            pltpu.VMEM((edges, 128), F32),
            pltpu.VMEM((edges, 128), jnp.int32),
            pltpu.VMEM((table, d), BF16),
            pltpu.VMEM((table, d), BF16),
            pltpu.VMEM((nodes, d), F32),
            pltpu.VMEM((nodes, d), BF16),
            pltpu.VMEM((nodes, d), F32),
            pltpu.VMEM((nodes, d), BF16),
            pltpu.VMEM((2, chunk, 128), F32),
            pltpu.VMEM((table, d), F32),
            pltpu.VMEM((d, d), F32),
            pltpu.VMEM((d, d), F32),
            pltpu.SemaphoreType.DMA((2, edges // chunk)),
            pltpu.SemaphoreType.DMA((2, edges // chunk)),
        ],
        compiler_params=params,
    )(
        node_latent,
        received,
        sender_slot,
        edge_mask,
        sender_slot.reshape(1, edges),
        w_edge_in,
        b_edge.reshape(1, d),
        w_edge_out,
        g_edge.reshape(1, d),
        w_node_in,
        b_node.reshape(1, d),
        w_node_out,
        g_node.reshape(1, d),
        node_cot,
        edge_latent,
        edge_cot,
    )
    pieces = [back[j * capacity : (j + 1) * capacity] for j in range(8)]
    arrived = jnp.concatenate(exchange(pieces, (("band", True), ("sector", True))))
    node_grad = pl.pallas_call(
        collect_kernel, out_shape=shape((nodes, d), F32), compiler_params=params
    )(send_rows.reshape(1, far), arrived, partial, w_edge_in[d : 2 * d])
    summed = summed_over_devices(grads).astype(F32) * (float(devices * edges) ** (-0.5))
    return (
        node_new,
        edge_new,
        node_grad,
        edge_grad,
        summed[: 3 * d],
        summed[3 * d : 4 * d],
        summed[4 * d : 6 * d],
        summed[6 * d :],
    )


def solution(mesh):
    split = P(("band", "sector"), None)
    in_specs = (split, split, split, split, P(("band", "sector"), None, None))
    in_specs += (P(),) * 8 + (split, split)
    out_specs = (split,) * 4 + (P(),) * 4
    return jax.shard_map(local, mesh=mesh, in_specs=in_specs, out_specs=out_specs, check_vma=False)
```

```python
import functools

import jax
import jax.numpy as jnp
from jax import lax
from jax.experimental import pallas as pl
from jax.experimental.pallas import tpu as pltpu
from jax.sharding import PartitionSpec as P

band_steps = (-1, -1, -1, 0, 0, 1, 1, 1)
sector_steps = (-1, 0, 1, -1, 1, -1, 0, 1)
AHEAD = tuple(j for j in range(8) if sector_steps[j] == 1)
BEHIND = tuple(j for j in range(8) if sector_steps[j] == -1)
SAME = tuple(j for j in range(8) if sector_steps[j] == 0)
UP = tuple(j for j in range(8) if band_steps[j] == 1)
DOWN = tuple(j for j in range(8) if band_steps[j] == -1)
LEVEL = tuple(j for j in range(8) if band_steps[j] == 0)
BF16 = jnp.bfloat16
F32 = jnp.float32


def shifted(array, axis, by):
    count = lax.axis_size(axis)
    return lax.ppermute(array, axis, [(i, (i + by) % count) for i in range(count)])


def flipped(array, mask):
    count = lax.axis_size("band") * lax.axis_size("sector")
    return lax.ppermute(array, ("band", "sector"), [(i, i ^ mask) for i in range(count)])


def position():
    return lax.axis_index("band") * lax.axis_size("sector") + lax.axis_index("sector")


def quarter(array, index):
    rows = array.shape[0] // 4
    return lax.dynamic_slice_in_dim(array, index * rows, rows, 0)


def plus(first, *others):
    total = first.astype(F32)
    for other in others:
        total = total + other.astype(F32)
    return total.astype(BF16)


def summed_halves(array, beside_first, beside_second):
    count = lax.axis_size("band") * lax.axis_size("sector")
    here = position()
    half = array.shape[0] // 2
    bit = here % 2
    give = lax.dynamic_slice_in_dim(array, (1 - bit) * half, half, 0)
    keep = lax.dynamic_slice_in_dim(array, bit * half, half, 0)
    held = plus(keep, flipped(give, 1))
    place = (here // 2) % 4
    got = [flipped(quarter(held, place ^ turn), 2 * turn) for turn in (3, 1, 2)]
    part = plus(quarter(held, place), *got)
    part, first = lax.optimization_barrier((part, beside_first()))
    second = beside_second(first)
    masks, step = [], 8
    while step < count:
        masks.append(step)
        step *= 2
    if len(masks) > 1:
        masks[1] |= masks[0]
    for mask in masks:
        part = plus(part, flipped(part, mask))
    part, second = lax.optimization_barrier((part, second))
    parts = {turn: flipped(part, 2 * turn) for turn in (3, 1, 2)}
    parts[0] = part
    rows = []
    for at in range(4):
        chosen = parts[at ^ 3]
        for turn in range(3):
            chosen = jnp.where(place == turn, parts[at ^ turn], chosen)
        rows.append(chosen)
    held = jnp.concatenate(rows)
    return held, flipped(held, 1), second


def dot(a, b, ca=1, cb=0):
    return lax.dot_general(a, b, (((ca,), (cb,)), ((), ())), preferred_element_type=F32)


def row_mean(values):
    return jnp.mean(values, axis=-1, keepdims=True)


def silu_parts(v):
    gate = 0.5 * jnp.tanh(0.5 * v) + 0.5
    out = v * gate
    return out, gate + out * (1.0 - gate)


def picked(rows_ref, count):
    rows = rows_ref[...]
    flat = jnp.concatenate([rows[j : j + 1, :] for j in range(rows.shape[0])], axis=1)
    lines = lax.broadcasted_iota(jnp.int32, (count, flat.shape[1]), 0)
    return jnp.where(flat == lines, 1.0, 0.0).astype(BF16)


def provide_kernel(rows_ref, node_ref, ahead_ref, behind_ref, same_ref):
    rows = dot(picked(rows_ref, node_ref.shape[0]), node_ref[...], 0, 0).astype(BF16)
    cap = rows_ref.shape[1]
    for ref, members in ((ahead_ref, AHEAD), (behind_ref, BEHIND), (same_ref, SAME)):
        for place, course in enumerate(members):
            ref[place * cap : (place + 1) * cap, :] = rows[course * cap : (course + 1) * cap, :]


def collect_kernel(rows_ref, ahead_ref, behind_ref, same_ref, partial_ref, w_ref, out_ref):
    cap = rows_ref.shape[1]
    pieces = {}
    for ref, members in ((ahead_ref, AHEAD), (behind_ref, BEHIND), (same_ref, SAME)):
        for place, course in enumerate(members):
            pieces[course] = ref[place * cap : (place + 1) * cap, :]
    arrived = jnp.concatenate([pieces[course] for course in range(8)])
    total = dot(picked(rows_ref, partial_ref.shape[0]), arrived).astype(BF16)
    out_ref[...] = partial_ref[...] + dot(total, w_ref[...], 1, 1)


def finish_kernel(bit_ref, held_ref, got_ref, in_ref, out_ref, node_in_ref, node_out_ref, *, scale):
    first = bit_ref[0] == 0
    held = held_ref[...].astype(F32) * scale
    got = got_ref[...].astype(F32) * scale
    halves = (jnp.where(first, held, got), jnp.where(first, got, held))
    half = held.shape[0]
    start = 0
    for ref in (in_ref, out_ref, node_in_ref, node_out_ref):
        rows = ref.shape[0]
        for side in range(2):
            lo, hi = max(start, side * half), min(start + rows, (side + 1) * half)
            if lo < hi:
                ref[lo - start : hi - start, :] = halves[side][lo - side * half : hi - side * half, :]
        start += rows


def pieces_of(chunk):
    def piece(index):
        return pl.ds(pl.multiple_of(index * chunk, chunk), chunk)

    return piece


def one_hot(values, lanes, first, last):
    parts = [jnp.where(values == lanes + at, 1.0, 0.0).astype(BF16) for at in range(first, last, 128)]
    return jnp.concatenate(parts, axis=1)


class Wide:
    def __init__(self, ref, slots):
        self.ref, self.slots = ref, slots
        self.blocks, self.rows = ref.shape[0], ref.shape[1] // slots

    def spread(self, rows):
        for k in range(self.slots):
            for block in range(self.blocks):
                part = rows[:, block * 128 : (block + 1) * 128]
                self.ref[block, pl.ds(k, self.rows, stride=self.slots), :] = part

    def get(self):
        return jnp.concatenate([self.ref[block] for block in range(self.blocks)], axis=1)

    def put(self, values):
        for block in range(self.blocks):
            self.ref[block] = values[:, block * 128 : (block + 1) * 128]

    def folded(self):
        parts = []
        for block in range(self.blocks):
            total = self.ref[block, pl.ds(0, self.rows, stride=self.slots), :]
            for k in range(1, self.slots):
                total = total + self.ref[block, pl.ds(k, self.rows, stride=self.slots), :]
            parts.append(total)
        return jnp.concatenate(parts, axis=1)


def near_kernel(
    slot_ref,
    mask_ref,
    b_edge_ref,
    after_ref,
    own_hbm,
    w_in_hbm,
    edge_hbm,
    near_hbm,
    code_hbm,
    own_v,
    w_in_v,
    edge_v,
    near_v,
    code_v,
    proj_v,
    recv_v,
    wide_v,
    sem_whole,
    sem_in,
    sem_out,
    *,
    chunk,
):
    nodes, d = own_v.shape
    edges = edge_v.shape[0]
    slots = edges // nodes
    count = edges // chunk
    cn = chunk // slots
    piece = pieces_of(chunk)
    wholes = [
        pltpu.make_async_copy(src, dst, sem_whole.at[place])
        for place, (src, dst) in enumerate(((own_hbm, own_v), (w_in_hbm, w_in_v)))
    ]
    for copy in wholes:
        copy.start()

    def pull(index):
        return pltpu.make_async_copy(edge_hbm.at[piece(index)], edge_v.at[piece(index)], sem_in.at[index])

    def push(kind, index):
        src, dst = ((near_v, near_hbm), (code_v, code_hbm))[kind]
        return pltpu.make_async_copy(src.at[piece(index)], dst.at[piece(index)], sem_out.at[kind, index])

    for index in range(count):
        pull(index).start()
    code = slot_ref[...] * 2 + mask_ref[...]
    for k in range(slots):
        code_v[pl.ds(k, nodes, stride=slots), :] = jnp.broadcast_to(code[:, k : k + 1], (nodes, 128))
    for copy in wholes:
        copy.wait()
    own = own_v[...]
    proj_v[...] = dot(own, w_in_v[d : 2 * d, :]).astype(BF16)
    recv_v[...] = dot(own, w_in_v[2 * d :, :]) + b_edge_ref[...]
    lanes = lax.broadcasted_iota(jnp.int32, (chunk, 128), 1)
    wide = Wide(wide_v, slots)

    def step(index, carry):
        rows = piece(index)
        pull(index).wait()
        wide.spread(recv_v[pl.ds(pl.multiple_of(index * cn, cn), cn), :])
        pick = one_hot(lax.shift_right_logical(code_v[rows, :], 1), lanes, 0, nodes)
        near_v[rows, :] = dot(edge_v[rows, :], w_in_v[:d, :]) + dot(pick, proj_v[...]) + wide.get()
        push(0, index).start()
        push(1, index).start()
        return carry

    lax.fori_loop(0, count, step, 0)
    for kind in range(2):
        for index in range(count):
            push(kind, index).wait()


def layer_kernel(
    slot_row_ref,
    g_edge_ref,
    b_node_ref,
    g_node_ref,
    up_ref,
    down_ref,
    ahead_ref,
    behind_ref,
    own_hbm,
    w_in_hbm,
    w_out_hbm,
    wn_in_hbm,
    wn_out_hbm,
    node_cot_hbm,
    edge_hbm,
    cot_hbm,
    near_hbm,
    code_hbm,
    node_new_ref,
    new_hbm,
    partial_ref,
    grad_hbm,
    up_back_ref,
    down_back_ref,
    level_back_ref,
    wg_ref,
    own_v,
    w_in_ref,
    w_out_ref,
    wn_in_ref,
    wn_out_ref,
    node_cot_v,
    edge_v,
    cot_v,
    near_v,
    code_v,
    new_v,
    grad_v,
    hid_v,
    slope_v,
    norm_v,
    scale_v,
    table_v,
    proj_v,
    gath_v,
    dgath_v,
    drecv_v,
    wide_v,
    t_acc,
    we_acc,
    wo_acc,
    sem_whole,
    sem_in,
    sem_out,
    *,
    chunk,
):
    nodes, d = own_v.shape
    edges = edge_v.shape[0]
    slots = edges // nodes
    cap = up_ref.shape[0] // 3
    table = nodes + 8 * cap
    count = edges // chunk
    cn = chunk // slots
    piece = pieces_of(chunk)

    def pull(kind, index):
        src, dst = ((near_hbm, near_v), (code_hbm, code_v), (edge_hbm, edge_v), (cot_hbm, cot_v))[kind]
        return pltpu.make_async_copy(src.at[piece(index)], dst.at[piece(index)], sem_in.at[kind, index])

    def push(kind, index):
        src, dst = ((new_v, new_hbm), (grad_v, grad_hbm))[kind]
        return pltpu.make_async_copy(src.at[piece(index)], dst.at[piece(index)], sem_out.at[kind, index])

    wholes = [
        pltpu.make_async_copy(src, dst, sem_whole.at[place])
        for place, (src, dst) in enumerate(
            (
                (w_in_hbm, w_in_ref),
                (w_out_hbm, w_out_ref),
                (own_hbm, own_v),
                (wn_in_hbm, wn_in_ref),
                (wn_out_hbm, wn_out_ref),
                (node_cot_hbm, node_cot_v),
            )
        )
    ]
    for copy in wholes[:2]:
        copy.start()
    for index in range(count):
        for kind in range(3):
            pull(kind, index).start()
    for copy in wholes[2:]:
        copy.start()
    for index in range(count):
        pull(3, index).start()

    level = (behind_ref[cap : 2 * cap, :], ahead_ref[cap : 2 * cap, :])
    for members, rows in ((UP, up_ref[...]), (DOWN, down_ref[...]), (LEVEL, jnp.concatenate(level))):
        for place, course in enumerate(members):
            at = nodes + course * cap
            table_v[at : at + cap, :] = rows[place * cap : (place + 1) * cap, :]
    for copy in wholes[:2]:
        copy.wait()
    proj_v[...] = dot(table_v[nodes:, :], w_in_ref[d : 2 * d, :]).astype(BF16)
    gain = g_edge_ref[...]
    lanes = lax.broadcasted_iota(jnp.int32, (chunk, 128), 1)
    wide = Wide(wide_v, slots)

    def part(index):
        return pl.ds(pl.multiple_of(index * cn, cn), cn)

    def ahead(index, carry):
        rows = piece(index)
        for kind in range(3):
            pull(kind, index).wait()
        code = code_v[rows, :]
        pick = one_hot(lax.shift_right_logical(code, 1), lanes, nodes, table)
        pre = near_v[rows, :] + dot(pick, proj_v[...])
        hidden, slope = silu_parts(pre)
        hidden = hidden.astype(BF16)
        hid_v[rows, :] = hidden
        slope_v[rows, :] = slope.astype(BF16)
        y = dot(hidden, w_out_ref[...])
        y = y - row_mean(y)
        rstd = lax.rsqrt(row_mean(y * y) + 1e-05)
        norm = y * rstd
        norm_v[rows, :] = norm.astype(BF16)
        valid = (code & 1).astype(F32)
        scale_v[rows, :] = valid * rstd
        update = norm * valid[:, :1] * gain
        new_v[rows, :] = (edge_v[rows, :].astype(F32) + update).astype(BF16)
        wide.put(update)
        gath_v[part(index), :] = wide.folded().astype(BF16)
        push(0, index).start()
        return carry

    lax.fori_loop(0, count, ahead, 0)

    for copy in wholes[2:]:
        copy.wait()
    own = own_v[...]
    table_v[:nodes, :] = own
    gathered = gath_v[...]
    pre = dot(own, wn_in_ref[:d, :]) + dot(gathered, wn_in_ref[d:, :]) + b_node_ref[...]
    hidden, slope = silu_parts(pre)
    hidden = hidden.astype(BF16)
    y = dot(hidden, wn_out_ref[...])
    y = y - row_mean(y)
    rstd = lax.rsqrt(row_mean(y * y) + 1e-05)
    norm = y * rstd
    node_new_ref[...] = (own.astype(F32) + norm * g_node_ref[...]).astype(BF16)
    node_cot = node_cot_v[...].astype(F32)
    a = node_cot * g_node_ref[...]
    dy = ((a - row_mean(a) - norm * row_mean(a * norm)) * rstd).astype(BF16)
    dpre = (dot(dy, wn_out_ref[...], 1, 1) * slope).astype(BF16)
    dgath_v[...] = dot(dpre, wn_in_ref[d:, :], 1, 1)
    partial_ref[...] = node_cot + dot(dpre, wn_in_ref[:d, :], 1, 1)
    wg_ref[4 * d : 5 * d, :] = dot(own, dpre, 0, 0).astype(BF16)
    wg_ref[5 * d : 6 * d, :] = dot(gathered, dpre, 0, 0).astype(BF16)
    wg_ref[6 * d : 7 * d, :] = dot(hidden, dy, 0, 0).astype(BF16)

    t_acc[...] = jnp.zeros_like(t_acc)
    we_acc[...] = jnp.zeros_like(we_acc)
    wo_acc[...] = jnp.zeros_like(wo_acc)
    lines = lax.broadcasted_iota(jnp.int32, (table, chunk), 0)

    def behind(index, carry):
        rows = piece(index)
        pull(3, index).wait()
        cot = cot_v[rows, :].astype(F32)
        wide.spread(dgath_v[part(index), :])
        a = (cot + wide.get()) * gain
        norm = norm_v[rows, :].astype(F32)
        dy = ((a - row_mean(a) - norm * row_mean(a * norm)) * scale_v[rows, :][:, :1]).astype(BF16)
        dpre = dot(dy, w_out_ref[...], 1, 1) * slope_v[rows, :].astype(F32)
        wide.put(dpre)
        drecv_v[part(index), :] = wide.folded().astype(BF16)
        dpre = dpre.astype(BF16)
        grad_v[rows, :] = (cot + dot(dpre, w_in_ref[:d, :], 1, 1)).astype(BF16)
        push(1, index).start()
        wo_acc[...] += dot(hid_v[rows, :], dy, 0, 0)
        we_acc[...] += dot(edge_v[rows, :], dpre, 0, 0)
        pick = jnp.where(slot_row_ref[:, rows] == lines, 1.0, 0.0).astype(BF16)
        t_acc[...] += dot(pick, dpre)
        return carry

    lax.fori_loop(0, count, behind, 0)

    total = t_acc[...].astype(BF16)
    for members, ref in ((UP, up_back_ref), (DOWN, down_back_ref), (LEVEL, level_back_ref)):
        for place, course in enumerate(members):
            at = nodes + course * cap
            ref[place * cap : (place + 1) * cap, :] = total[at : at + cap, :]
    drecv = drecv_v[...]
    partial_ref[...] += dot(total[:nodes, :], w_in_ref[d : 2 * d, :], 1, 1) + dot(drecv, w_in_ref[2 * d :, :], 1, 1)
    wg_ref[:d, :] = we_acc[...].astype(BF16)
    wg_ref[d : 2 * d, :] = dot(table_v[...], total, 0, 0).astype(BF16)
    wg_ref[2 * d : 3 * d, :] = dot(own, drecv, 0, 0).astype(BF16)
    wg_ref[3 * d : 4 * d, :] = wo_acc[...].astype(BF16)
    for kind in range(2):
        for index in range(count):
            push(kind, index).wait()


def local(
    node_latent,
    edge_latent,
    sender_slot,
    edge_mask,
    send_rows,
    w_edge_in,
    b_edge,
    w_edge_out,
    g_edge,
    w_node_in,
    b_node,
    w_node_out,
    g_node,
    node_cot,
    edge_cot,
):
    nodes, d = node_latent.shape
    edges = edge_latent.shape[0]
    slots = sender_slot.shape[1]
    capacity = send_rows.shape[2]
    far = 8 * capacity
    table = nodes + far
    devices = lax.axis_size("band") * lax.axis_size("sector")
    params = pltpu.CompilerParams(vmem_limit_bytes=50 * 1024 * 1024)
    shape = jax.ShapeDtypeStruct
    rows = send_rows.reshape(8, capacity)
    ahead, behind, same = pl.pallas_call(
        provide_kernel,
        out_shape=tuple(shape((len(m) * capacity, d), BF16) for m in (AHEAD, BEHIND, SAME)),
        compiler_params=params,
    )(rows, node_latent)

    def course_of(course, sets):
        for members, block in sets:
            if course in members:
                at = members.index(course) * capacity
                return block[at : at + capacity]

    def gathered_rows(courses, sets):
        return jnp.concatenate([course_of(course, sets) for course in courses])

    ahead, behind = shifted(ahead, "sector", -1), shifted(behind, "sector", 1)
    sets = ((AHEAD, ahead), (BEHIND, behind), (SAME, same))
    up = shifted(gathered_rows(UP, sets), "band", -1)
    down = shifted(gathered_rows(DOWN, sets), "band", 1)

    chunk = 64 * slots
    count = edges // chunk
    vmem = pl.BlockSpec(memory_space=pltpu.VMEM)
    hbm = pl.BlockSpec(memory_space=pltpu.HBM)
    free = pl.BlockSpec(memory_space=pl.ANY)
    dma = pltpu.SemaphoreType.DMA
    near, code = pl.pallas_call(
        functools.partial(near_kernel, chunk=chunk),
        out_shape=(shape((edges, d), F32), shape((edges, 128), jnp.int32)),
        in_specs=[vmem] * 3 + [free] + [hbm] * 3,
        out_specs=(hbm,) * 2,
        scratch_shapes=[
            pltpu.VMEM((nodes, d), BF16),
            pltpu.VMEM(w_edge_in.shape, BF16),
            pltpu.VMEM((edges, d), BF16),
            pltpu.VMEM((edges, d), F32),
            pltpu.VMEM((edges, 128), jnp.int32),
            pltpu.VMEM((nodes, d), BF16),
            pltpu.VMEM((nodes, d), F32),
            pltpu.VMEM((d // 128, chunk, 128), F32),
            dma((2,)),
            dma((count,)),
            dma((2, count)),
        ],
        compiler_params=params,
        cost_estimate=pl.CostEstimate(flops=6 * edges * d * d, transcendentals=0, bytes_accessed=16 * edges * d),
    )(sender_slot, edge_mask, b_edge.reshape(1, d), ahead, node_latent, w_edge_in, edge_latent)
    node_new, edge_new, partial, edge_grad, up_back, down_back, level_back, grads = pl.pallas_call(
        functools.partial(layer_kernel, chunk=chunk),
        out_shape=(
            shape((nodes, d), BF16),
            shape((edges, d), BF16),
            shape((nodes, d), F32),
            shape((edges, d), BF16),
            shape((3 * capacity, d), BF16),
            shape((3 * capacity, d), BF16),
            shape((2 * capacity, d), BF16),
            shape((7 * d, d), BF16),
        ),
        in_specs=[vmem] * 8 + [hbm] * 10,
        out_specs=(vmem, hbm, vmem, hbm, vmem, vmem, vmem, vmem),
        scratch_shapes=[
            pltpu.VMEM((nodes, d), BF16),
            pltpu.VMEM(w_edge_in.shape, BF16),
            pltpu.VMEM(w_edge_out.shape, BF16),
            pltpu.VMEM(w_node_in.shape, BF16),
            pltpu.VMEM(w_node_out.shape, BF16),
            pltpu.VMEM((nodes, d), BF16),
            pltpu.VMEM((edges, d), BF16),
            pltpu.VMEM((edges, d), BF16),
            pltpu.VMEM((edges, d), F32),
            pltpu.VMEM((edges, 128), jnp.int32),
            pltpu.VMEM((edges, d), BF16),
            pltpu.VMEM((edges, d), BF16),
            pltpu.VMEM((edges, d), BF16),
            pltpu.VMEM((edges, d), BF16),
            pltpu.VMEM((edges, d), BF16),
            pltpu.VMEM((edges, 128), F32),
            pltpu.VMEM((table, d), BF16),
            pltpu.VMEM((far, d), BF16),
            pltpu.VMEM((nodes, d), BF16),
            pltpu.VMEM((nodes, d), F32),
            pltpu.VMEM((nodes, d), BF16),
            pltpu.VMEM((d // 128, chunk, 128), F32),
            pltpu.VMEM((table, d), F32),
            pltpu.VMEM((d, d), F32),
            pltpu.VMEM((d, d), F32),
            dma((6,)),
            dma((4, count)),
            dma((2, count)),
        ],
        compiler_params=params,
    )(
        sender_slot.reshape(1, edges),
        g_edge.reshape(1, d),
        b_node.reshape(1, d),
        g_node.reshape(1, d),
        up,
        down,
        ahead,
        behind,
        node_latent,
        w_edge_in,
        w_edge_out,
        w_node_in,
        w_node_out,
        node_cot,
        edge_latent,
        edge_cot,
        near,
        code,
    )

    def return_bands():
        return shifted(up_back, "band", 1), shifted(down_back, "band", -1)

    def return_sectors(moved):
        sets = ((UP, moved[0]), (DOWN, moved[1]), (LEVEL, level_back))
        ahead = shifted(gathered_rows(AHEAD, sets), "sector", 1)
        behind = shifted(gathered_rows(BEHIND, sets), "sector", -1)
        return ahead, behind, gathered_rows(SAME, sets)

    held, got, (ahead, behind, same) = summed_halves(grads, return_bands, return_sectors)
    whole = lambda *dims: pl.BlockSpec(dims, lambda i: (0,) * len(dims))
    node_grad = pl.pallas_call(
        collect_kernel,
        grid=(1,),
        in_specs=[
            whole(8, capacity),
            whole(3 * capacity, d),
            whole(3 * capacity, d),
            whole(2 * capacity, d),
            whole(nodes, d),
            pl.BlockSpec((d, d), lambda i: (1, 0)),
        ],
        out_specs=whole(nodes, d),
        out_shape=shape((nodes, d), F32),
        compiler_params=params,
    )(rows, ahead, behind, same, partial, w_edge_in)
    grad_in, grad_out, grad_node_in, grad_node_out = pl.pallas_call(
        functools.partial(finish_kernel, scale=float(devices * edges) ** (-0.5)),
        in_specs=[pl.BlockSpec(memory_space=pltpu.SMEM), vmem, vmem],
        out_specs=(vmem,) * 4,
        out_shape=tuple(shape((parts * d, d), F32) for parts in (3, 1, 2, 1)),
        compiler_params=params,
    )((position() % 2).reshape(1), held, got)
    return (node_new, edge_new, node_grad, edge_grad, grad_in, grad_out, grad_node_in, grad_node_out)


def solution(mesh):
    split = P(("band", "sector"), None)
    in_specs = (split, split, split, split, P(("band", "sector"), None, None))
    in_specs += (P(),) * 8 + (split, split)
    out_specs = (split,) * 4 + (P(),) * 4
    return jax.shard_map(local, mesh=mesh, in_specs=in_specs, out_specs=out_specs, check_vma=False)
```

```python
import functools

import jax
import jax.numpy as jnp
from jax import lax
from jax.experimental import pallas as pl
from jax.experimental.pallas import tpu as pltpu
from jax.sharding import PartitionSpec as P

band_steps = (-1, -1, -1, 0, 0, 1, 1, 1)
sector_steps = (-1, 0, 1, -1, 1, -1, 0, 1)
AHEAD = tuple(j for j in range(8) if sector_steps[j] == 1)
BEHIND = tuple(j for j in range(8) if sector_steps[j] == -1)
SAME = tuple(j for j in range(8) if sector_steps[j] == 0)
UP = tuple(j for j in range(8) if band_steps[j] == 1)
DOWN = tuple(j for j in range(8) if band_steps[j] == -1)
LEVEL = tuple(j for j in range(8) if band_steps[j] == 0)
BF16 = jnp.bfloat16
F32 = jnp.float32


def shifted(array, axis, by):
    count = lax.axis_size(axis)
    return lax.ppermute(array, axis, [(i, (i + by) % count) for i in range(count)])


def flipped(array, mask):
    count = lax.axis_size("band") * lax.axis_size("sector")
    return lax.ppermute(array, ("band", "sector"), [(i, i ^ mask) for i in range(count)])


def position():
    return lax.axis_index("band") * lax.axis_size("sector") + lax.axis_index("sector")


def quarter(array, index):
    rows = array.shape[0] // 4
    return lax.dynamic_slice_in_dim(array, index * rows, rows, 0)


def plus(first, *others):
    total = first.astype(F32)
    for other in others:
        total = total + other.astype(F32)
    return total.astype(BF16)


def summed_halves(array, beside_first, beside_second):
    count = lax.axis_size("band") * lax.axis_size("sector")
    here = position()
    half = array.shape[0] // 2
    bit = here % 2
    give = lax.dynamic_slice_in_dim(array, (1 - bit) * half, half, 0)
    keep = lax.dynamic_slice_in_dim(array, bit * half, half, 0)
    held = plus(keep, flipped(give, 1))
    place = (here // 2) % 4
    got = [flipped(quarter(held, place ^ turn), 2 * turn) for turn in (3, 1, 2)]
    part = plus(quarter(held, place), *got)
    part, first = lax.optimization_barrier((part, beside_first()))
    second = beside_second(first)
    masks, step = [], 8
    while step < count:
        masks.append(step)
        step *= 2
    if len(masks) > 1:
        masks[1] |= masks[0]
    for mask in masks:
        part = plus(part, flipped(part, mask))
    part, second = lax.optimization_barrier((part, second))
    parts = {turn: flipped(part, 2 * turn) for turn in (3, 1, 2)}
    parts[0] = part
    rows = []
    for at in range(4):
        chosen = parts[at ^ 3]
        for turn in range(3):
            chosen = jnp.where(place == turn, parts[at ^ turn], chosen)
        rows.append(chosen)
    held = jnp.concatenate(rows)
    return held, flipped(held, 1), second


def dot(a, b, ca=1, cb=0):
    return lax.dot_general(a, b, (((ca,), (cb,)), ((), ())), preferred_element_type=F32)


def doubled(values):
    return jnp.concatenate([values, values], axis=1)


def row_mean(values):
    return jnp.mean(values, axis=-1, keepdims=True)


def silu_parts(v):
    gate = 0.5 * jnp.tanh(0.5 * v) + 0.5
    out = v * gate
    return out, gate + out * (1.0 - gate)


def picked(rows_ref, count):
    rows = rows_ref[...]
    flat = jnp.concatenate([rows[j : j + 1, :] for j in range(rows.shape[0])], axis=1)
    lines = lax.broadcasted_iota(jnp.int32, (count, flat.shape[1]), 0)
    return jnp.where(flat == lines, 1.0, 0.0).astype(BF16)


def provide_kernel(rows_ref, node_hbm, w_hbm, ahead_ref, behind_ref, same_ref, own_ref, w_ref, sem):
    copies = [
        pltpu.make_async_copy(src, dst, sem.at[place])
        for place, (src, dst) in enumerate(((node_hbm, own_ref), (w_hbm, w_ref)))
    ]
    for copy in copies:
        copy.start()
    pick = picked(rows_ref, own_ref.shape[0])
    copies[0].wait()
    rows = dot(pick, own_ref[...], 0, 0).astype(BF16)
    cap = rows_ref.shape[1]
    for ref, members in ((ahead_ref, AHEAD), (behind_ref, BEHIND), (same_ref, SAME)):
        for place, course in enumerate(members):
            ref[place * cap : (place + 1) * cap, :] = rows[course * cap : (course + 1) * cap, :]
    copies[1].wait()


def collect_kernel(rows_ref, ahead_ref, behind_ref, same_ref, partial_ref, w_ref, out_ref):
    cap = rows_ref.shape[1]
    pieces = {}
    for ref, members in ((ahead_ref, AHEAD), (behind_ref, BEHIND), (same_ref, SAME)):
        for place, course in enumerate(members):
            pieces[course] = ref[place * cap : (place + 1) * cap, :]
    arrived = jnp.concatenate([pieces[course] for course in range(8)])
    total = dot(picked(rows_ref, partial_ref.shape[0]), arrived).astype(BF16)
    out_ref[...] = partial_ref[...] + dot(total, w_ref[...], 1, 1)


def finish_kernel(bit_ref, held_ref, got_ref, in_ref, out_ref, node_in_ref, node_out_ref, *, scale):
    first = bit_ref[0] == 0
    held = held_ref[...].astype(F32) * scale
    got = got_ref[...].astype(F32) * scale
    halves = (jnp.where(first, held, got), jnp.where(first, got, held))
    half = held.shape[0]
    start = 0
    for ref in (in_ref, out_ref, node_in_ref, node_out_ref):
        rows = ref.shape[0]
        for side in range(2):
            lo, hi = max(start, side * half), min(start + rows, (side + 1) * half)
            if lo < hi:
                ref[lo - start : hi - start, :] = halves[side][lo - side * half : hi - side * half, :]
        start += rows


def pieces_of(chunk):
    def piece(index):
        return pl.ds(pl.multiple_of(index * chunk, chunk), chunk)

    return piece


def one_hot(values, lanes, first, last):
    parts = [jnp.where(values == lanes + at, 1.0, 0.0).astype(BF16) for at in range(first, last, 128)]
    return jnp.concatenate(parts, axis=1)


class Wide:
    def __init__(self, ref, slots):
        self.ref, self.slots = ref, slots
        self.blocks, self.rows = ref.shape[0], ref.shape[1] // slots

    def spread(self, rows):
        for k in range(self.slots):
            for block in range(self.blocks):
                part = rows[:, block * 128 : (block + 1) * 128]
                self.ref[block, pl.ds(k, self.rows, stride=self.slots), :] = part

    def get(self):
        return jnp.concatenate([self.ref[block] for block in range(self.blocks)], axis=1)

    def put(self, values):
        for block in range(self.blocks):
            self.ref[block] = values[:, block * 128 : (block + 1) * 128]

    def folded(self):
        parts = []
        for block in range(self.blocks):
            total = self.ref[block, pl.ds(0, self.rows, stride=self.slots), :]
            for k in range(1, self.slots):
                total = total + self.ref[block, pl.ds(k, self.rows, stride=self.slots), :]
            parts.append(total)
        return jnp.concatenate(parts, axis=1)


def near_kernel(
    slot_ref,
    mask_ref,
    b_edge_ref,
    after_ref,
    own_ref,
    w_in_ref,
    edge_hbm,
    near_ref,
    code_ref,
    edge_ref,
    proj_v,
    recv_v,
    wide_v,
    sem_in,
    *,
    chunk,
):
    nodes, d = own_ref.shape
    edges = edge_ref.shape[0]
    slots = edges // nodes
    count = edges // chunk
    cn = chunk // slots
    piece = pieces_of(chunk)

    def pull(index):
        return pltpu.make_async_copy(edge_hbm.at[piece(index)], edge_ref.at[piece(index)], sem_in.at[index])

    for index in range(count):
        pull(index).start()
    code = slot_ref[...] * 2 + mask_ref[...]
    for k in range(slots):
        code_ref[pl.ds(k, nodes, stride=slots), :] = jnp.broadcast_to(code[:, k : k + 1], (nodes, 128))
    own = own_ref[...]
    proj_v[...] = dot(own, w_in_ref[d : 2 * d, :]).astype(BF16)
    recv_v[...] = dot(own, w_in_ref[2 * d :, :]) + b_edge_ref[...]
    lanes = lax.broadcasted_iota(jnp.int32, (chunk, 128), 1)
    wide = Wide(wide_v, slots)

    def step(index, carry):
        rows = piece(index)
        pull(index).wait()
        wide.spread(recv_v[pl.ds(pl.multiple_of(index * cn, cn), cn), :])
        pick = one_hot(lax.shift_right_logical(code_ref[rows, :], 1), lanes, 0, nodes)
        near_ref[rows, :] = 0.5 * (dot(edge_ref[rows, :], w_in_ref[:d, :]) + dot(pick, proj_v[...]) + wide.get())
        return carry

    lax.fori_loop(0, count, step, 0)


def layer_kernel(
    slot_row_ref,
    g_edge_ref,
    b_node_ref,
    g_node_ref,
    up_ref,
    down_ref,
    ahead_ref,
    behind_ref,
    own_ref,
    w_in_ref,
    near_v,
    code_v,
    edge_v,
    w_out_hbm,
    wn_in_hbm,
    wn_out_hbm,
    node_cot_hbm,
    cot_hbm,
    node_new_ref,
    new_hbm,
    partial_ref,
    grad_hbm,
    up_back_ref,
    down_back_ref,
    level_back_ref,
    wg_ref,
    w_out_ref,
    wn_in_ref,
    wn_out_ref,
    node_cot_v,
    cot_v,
    new_v,
    grad_v,
    hid_v,
    slope_v,
    norm_v,
    scale_v,
    table_v,
    proj_v,
    gath_v,
    dgath_v,
    drecv_v,
    wide_v,
    t_acc,
    we_acc,
    wo_acc,
    back_v,
    dy_v,
    dpre_v,
    sem_whole,
    sem_in,
    sem_out,
    *,
    chunk,
):
    nodes, d = own_ref.shape
    edges = edge_v.shape[0]
    slots = edges // nodes
    cap = up_ref.shape[0] // 3
    table = nodes + 8 * cap
    count = edges // chunk
    cn = chunk // slots
    piece = pieces_of(chunk)

    def pull(index):
        return pltpu.make_async_copy(cot_hbm.at[piece(index)], cot_v.at[piece(index)], sem_in.at[index])

    def push(kind, index):
        src, dst = ((new_v, new_hbm), (grad_v, grad_hbm))[kind]
        return pltpu.make_async_copy(src.at[piece(index)], dst.at[piece(index)], sem_out.at[kind, index])

    wholes = [
        pltpu.make_async_copy(src, dst, sem_whole.at[place])
        for place, (src, dst) in enumerate(
            (
                (w_out_hbm, w_out_ref),
                (wn_in_hbm, wn_in_ref),
                (wn_out_hbm, wn_out_ref),
                (node_cot_hbm, node_cot_v),
            )
        )
    ]
    for copy in wholes:
        copy.start()
    for index in range(count):
        pull(index).start()

    level = (behind_ref[cap : 2 * cap, :], ahead_ref[cap : 2 * cap, :])
    for members, rows in ((UP, up_ref[...]), (DOWN, down_ref[...]), (LEVEL, jnp.concatenate(level))):
        for place, course in enumerate(members):
            at = nodes + course * cap
            table_v[at : at + cap, :] = rows[place * cap : (place + 1) * cap, :]
    proj_v[...] = (0.5 * dot(table_v[nodes:, :], w_in_ref[d : 2 * d, :])).astype(BF16)
    wholes[0].wait()
    back_v[...] = 0.5 * w_out_ref[...]
    gain = g_edge_ref[...]
    lanes = lax.broadcasted_iota(jnp.int32, (chunk, 128), 1)
    wides = (Wide(wide_v.at[0], slots), Wide(wide_v.at[1], slots))
    wide = wides[0]

    def part(index):
        return pl.ds(pl.multiple_of(index * cn, cn), cn)

    def ahead(index, carry):
        rows = piece(index)
        code = code_v[rows, :]
        pick = one_hot(lax.shift_right_logical(code, 1), lanes, nodes, table)
        half = near_v[rows, :] + dot(pick, proj_v[...])
        bend = jnp.tanh(half)
        gate = bend + 1.0
        hidden = half * gate
        slope_v[rows, :] = (gate + hidden * (1.0 - bend)).astype(BF16)
        hidden = hidden.astype(BF16)
        hid_v[rows, :] = hidden
        y = dot(hidden, w_out_ref[...])
        y = y - row_mean(y)
        rstd = lax.rsqrt(row_mean(y * y) + 1e-05)
        scale = (code & 1).astype(F32) * rstd
        scale_v[rows, :] = scale
        norm = y * doubled(scale)
        norm_v[rows, :] = norm.astype(BF16)
        update = norm * gain
        new_v[rows, :] = (edge_v[rows, :].astype(F32) + update).astype(BF16)
        wide.put(update)
        gath_v[part(index), :] = wide.folded().astype(BF16)
        push(0, index).start()
        return carry

    lax.fori_loop(0, count, ahead, 0)

    for copy in wholes[1:]:
        copy.wait()
    own = own_ref[...]
    table_v[:nodes, :] = own
    gathered = gath_v[...]
    pre = dot(own, wn_in_ref[:d, :]) + dot(gathered, wn_in_ref[d:, :]) + b_node_ref[...]
    hidden, slope = silu_parts(pre)
    hidden = hidden.astype(BF16)
    y = dot(hidden, wn_out_ref[...])
    y = y - row_mean(y)
    rstd = lax.rsqrt(row_mean(y * y) + 1e-05)
    norm = y * rstd
    node_new_ref[...] = (own.astype(F32) + norm * g_node_ref[...]).astype(BF16)
    node_cot = node_cot_v[...].astype(F32)
    a = node_cot * g_node_ref[...]
    dy = ((a - row_mean(a) - norm * row_mean(a * norm)) * rstd).astype(BF16)
    dpre = (dot(dy, wn_out_ref[...], 1, 1) * slope).astype(BF16)
    dgath_v[...] = dot(dpre, wn_in_ref[d:, :], 1, 1)
    partial_ref[...] = node_cot + dot(dpre, wn_in_ref[:d, :], 1, 1)
    wg_ref[4 * d : 5 * d, :] = dot(own, dpre, 0, 0).astype(BF16)
    wg_ref[5 * d : 6 * d, :] = dot(gathered, dpre, 0, 0).astype(BF16)
    wg_ref[6 * d : 7 * d, :] = dot(hidden, dy, 0, 0).astype(BF16)

    t_acc[...] = jnp.zeros_like(t_acc)
    we_acc[...] = jnp.zeros_like(we_acc)
    wo_acc[...] = jnp.zeros_like(wo_acc)
    lines = lax.broadcasted_iota(jnp.int32, (table, chunk), 0)

    def lead(index, side):
        rows = piece(index)
        cot = cot_v[rows, :].astype(F32)
        buffer = wides[side]
        buffer.spread(dgath_v[part(index), :])
        a = (cot + buffer.get()) * gain
        norm = norm_v[rows, :].astype(F32)
        dy = ((a - row_mean(a) - norm * row_mean(a * norm)) * doubled(scale_v[rows, :])).astype(BF16)
        dpre = dot(dy, back_v[...], 1, 1) * slope_v[rows, :].astype(F32)
        buffer.put(dpre)
        drecv_v[part(index), :] = buffer.folded().astype(BF16)
        dy_v[side] = dy
        dpre_v[side] = dpre.astype(BF16)

    def trail(index, side):
        rows = piece(index)
        dy, dpre = dy_v[side], dpre_v[side]
        grad_v[rows, :] = (cot_v[rows, :].astype(F32) + dot(dpre, w_in_ref[:d, :], 1, 1)).astype(BF16)
        wo_acc[...] += dot(hid_v[rows, :], dy, 0, 0)
        we_acc[...] += dot(edge_v[rows, :], dpre, 0, 0)
        pick = jnp.where(slot_row_ref[:, rows] == lines, 1.0, 0.0).astype(BF16)
        t_acc[...] += dot(pick, dpre)

    for index in range(count):
        pull(index).wait()
    lead(0, 0)

    def behind(pair, carry):
        trail(2 * pair, 0)
        lead(2 * pair + 1, 1)
        push(1, 2 * pair).start()
        trail(2 * pair + 1, 1)
        lead(jnp.minimum(2 * pair + 2, count - 1), 0)
        push(1, 2 * pair + 1).start()
        return carry

    lax.fori_loop(0, count // 2, behind, 0)

    total = t_acc[...].astype(BF16)
    for members, ref in ((UP, up_back_ref), (DOWN, down_back_ref), (LEVEL, level_back_ref)):
        for place, course in enumerate(members):
            at = nodes + course * cap
            ref[place * cap : (place + 1) * cap, :] = total[at : at + cap, :]
    drecv = drecv_v[...]
    partial_ref[...] += dot(total[:nodes, :], w_in_ref[d : 2 * d, :], 1, 1) + dot(drecv, w_in_ref[2 * d :, :], 1, 1)
    wg_ref[:d, :] = we_acc[...].astype(BF16)
    wg_ref[d : 2 * d, :] = dot(table_v[...], total, 0, 0).astype(BF16)
    wg_ref[2 * d : 3 * d, :] = dot(own, drecv, 0, 0).astype(BF16)
    wg_ref[3 * d : 4 * d, :] = wo_acc[...].astype(BF16)
    for kind in range(2):
        for index in range(count):
            push(kind, index).wait()


def local(
    node_latent,
    edge_latent,
    sender_slot,
    edge_mask,
    send_rows,
    w_edge_in,
    b_edge,
    w_edge_out,
    g_edge,
    w_node_in,
    b_node,
    w_node_out,
    g_node,
    node_cot,
    edge_cot,
):
    nodes, d = node_latent.shape
    edges = edge_latent.shape[0]
    slots = sender_slot.shape[1]
    capacity = send_rows.shape[2]
    far = 8 * capacity
    table = nodes + far
    devices = lax.axis_size("band") * lax.axis_size("sector")
    params = pltpu.CompilerParams(vmem_limit_bytes=34 * 1024 * 1024)
    shape = jax.ShapeDtypeStruct
    rows = send_rows.reshape(8, capacity)
    vmem = pl.BlockSpec(memory_space=pltpu.VMEM)
    hbm = pl.BlockSpec(memory_space=pltpu.HBM)
    free = pl.BlockSpec(memory_space=pl.ANY)
    dma = pltpu.SemaphoreType.DMA

    def off_chip(array):
        return pltpu.with_memory_space_constraint(array, pltpu.HBM)

    def on_chip(array):
        return pltpu.with_memory_space_constraint(array, pltpu.VMEM)

    w_shape = w_edge_in.shape
    ahead, behind, same, own, w_in = pl.pallas_call(
        provide_kernel,
        in_specs=[vmem, hbm, hbm],
        out_specs=(vmem,) * 5,
        out_shape=tuple(pltpu.VMEM((len(m) * capacity, d), BF16) for m in (AHEAD, BEHIND, SAME))
        + (pltpu.VMEM((nodes, d), BF16), pltpu.VMEM(w_shape, BF16)),
        scratch_shapes=[dma((2,))],
        compiler_params=params,
    )(rows, off_chip(node_latent), off_chip(w_edge_in))

    def course_of(course, sets):
        for members, block in sets:
            if course in members:
                at = members.index(course) * capacity
                return block[at : at + capacity]

    def gathered_rows(courses, sets):
        return jnp.concatenate([course_of(course, sets) for course in courses])

    ahead, behind = shifted(ahead, "sector", -1), shifted(behind, "sector", 1)
    sets = ((AHEAD, ahead), (BEHIND, behind), (SAME, same))
    up = shifted(gathered_rows(UP, sets), "band", -1)
    down = shifted(gathered_rows(DOWN, sets), "band", 1)

    chunk = 64 * slots
    count = edges // chunk
    near, code, edge = pl.pallas_call(
        functools.partial(near_kernel, chunk=chunk),
        out_shape=(pltpu.VMEM((edges, d), F32), pltpu.VMEM((edges, 128), jnp.int32), pltpu.VMEM((edges, d), BF16)),
        in_specs=[vmem] * 3 + [free] + [vmem] * 2 + [hbm],
        out_specs=(vmem,) * 3,
        scratch_shapes=[
            pltpu.VMEM((nodes, d), BF16),
            pltpu.VMEM((nodes, d), F32),
            pltpu.VMEM((d // 128, chunk, 128), F32),
            dma((count,)),
        ],
        compiler_params=params,
        cost_estimate=pl.CostEstimate(flops=6 * edges * d * d, transcendentals=0, bytes_accessed=16 * edges * d),
    )(sender_slot, edge_mask, b_edge.reshape(1, d), ahead, on_chip(own), on_chip(w_in), off_chip(edge_latent))
    node_new, edge_new, partial, edge_grad, up_back, down_back, level_back, grads = pl.pallas_call(
        functools.partial(layer_kernel, chunk=chunk),
        out_shape=(
            shape((nodes, d), BF16),
            shape((edges, d), BF16),
            pltpu.VMEM((nodes, d), F32),
            shape((edges, d), BF16),
            pltpu.VMEM((3 * capacity, d), BF16),
            pltpu.VMEM((3 * capacity, d), BF16),
            pltpu.VMEM((2 * capacity, d), BF16),
            pltpu.VMEM((7 * d, d), BF16),
        ),
        in_specs=[vmem] * 13 + [hbm] * 5,
        out_specs=(vmem, hbm, vmem, hbm, vmem, vmem, vmem, vmem),
        scratch_shapes=[
            pltpu.VMEM(w_edge_out.shape, BF16),
            pltpu.VMEM(w_node_in.shape, BF16),
            pltpu.VMEM(w_node_out.shape, BF16),
            pltpu.VMEM((nodes, d), BF16),
            pltpu.VMEM((edges, d), BF16),
            pltpu.VMEM((edges, d), BF16),
            pltpu.VMEM((edges, d), BF16),
            pltpu.VMEM((edges, d), BF16),
            pltpu.VMEM((edges, d), BF16),
            pltpu.VMEM((edges, d), BF16),
            pltpu.VMEM((edges, 128), F32),
            pltpu.VMEM((table, d), BF16),
            pltpu.VMEM((far, d), BF16),
            pltpu.VMEM((nodes, d), BF16),
            pltpu.VMEM((nodes, d), F32),
            pltpu.VMEM((nodes, d), BF16),
            pltpu.VMEM((2, d // 128, chunk, 128), F32),
            pltpu.VMEM((table, d), F32),
            pltpu.VMEM((d, d), F32),
            pltpu.VMEM((d, d), F32),
            pltpu.VMEM((d, d), BF16),
            pltpu.VMEM((2, chunk, d), BF16),
            pltpu.VMEM((2, chunk, d), BF16),
            dma((4,)),
            dma((count,)),
            dma((2, count)),
        ],
        compiler_params=params,
    )(
        sender_slot.reshape(1, edges),
        g_edge.reshape(1, d),
        b_node.reshape(1, d),
        g_node.reshape(1, d),
        up,
        down,
        ahead,
        behind,
        on_chip(own),
        on_chip(w_in),
        on_chip(near),
        on_chip(code),
        on_chip(edge),
        off_chip(w_edge_out),
        off_chip(w_node_in),
        off_chip(w_node_out),
        off_chip(node_cot),
        off_chip(edge_cot),
    )

    def return_bands():
        return shifted(up_back, "band", 1), shifted(down_back, "band", -1)

    def return_sectors(moved):
        sets = ((UP, moved[0]), (DOWN, moved[1]), (LEVEL, level_back))
        ahead = shifted(gathered_rows(AHEAD, sets), "sector", 1)
        behind = shifted(gathered_rows(BEHIND, sets), "sector", -1)
        return ahead, behind, gathered_rows(SAME, sets)

    held, got, (ahead, behind, same) = summed_halves(grads, return_bands, return_sectors)
    whole = lambda *dims: pl.BlockSpec(dims, lambda i: (0,) * len(dims))
    node_grad = pl.pallas_call(
        collect_kernel,
        grid=(1,),
        in_specs=[
            whole(8, capacity),
            whole(3 * capacity, d),
            whole(3 * capacity, d),
            whole(2 * capacity, d),
            whole(nodes, d),
            pl.BlockSpec((d, d), lambda i: (1, 0)),
        ],
        out_specs=whole(nodes, d),
        out_shape=shape((nodes, d), F32),
        compiler_params=params,
    )(rows, ahead, behind, same, partial, w_in)
    grad_in, grad_out, grad_node_in, grad_node_out = pl.pallas_call(
        functools.partial(finish_kernel, scale=float(devices * edges) ** (-0.5)),
        in_specs=[pl.BlockSpec(memory_space=pltpu.SMEM), vmem, vmem],
        out_specs=(vmem,) * 4,
        out_shape=tuple(shape((parts * d, d), F32) for parts in (3, 1, 2, 1)),
        compiler_params=params,
    )((position() % 2).reshape(1), held, got)
    return (node_new, edge_new, node_grad, edge_grad, grad_in, grad_out, grad_node_in, grad_node_out)


def solution(mesh):
    split = P(("band", "sector"), None)
    in_specs = (split, split, split, split, P(("band", "sector"), None, None))
    in_specs += (P(),) * 8 + (split, split)
    out_specs = (split,) * 4 + (P(),) * 4
    return jax.shard_map(local, mesh=mesh, in_specs=in_specs, out_specs=out_specs, check_vma=False)
```

```python
import functools

import jax
import jax.numpy as jnp
from jax import lax
from jax.experimental import pallas as pl
from jax.experimental.pallas import tpu as pltpu
from jax.sharding import PartitionSpec as P

band_steps = (-1, -1, -1, 0, 0, 1, 1, 1)
sector_steps = (-1, 0, 1, -1, 1, -1, 0, 1)
AHEAD = tuple(j for j in range(8) if sector_steps[j] == 1)
BEHIND = tuple(j for j in range(8) if sector_steps[j] == -1)
SAME = tuple(j for j in range(8) if sector_steps[j] == 0)
UP = tuple(j for j in range(8) if band_steps[j] == 1)
DOWN = tuple(j for j in range(8) if band_steps[j] == -1)
LEVEL = tuple(j for j in range(8) if band_steps[j] == 0)
BF16 = jnp.bfloat16
F32 = jnp.float32


def shifted(array, axis, by):
    count = lax.axis_size(axis)
    return lax.ppermute(array, axis, [(i, (i + by) % count) for i in range(count)])


def flipped(array, mask):
    count = lax.axis_size("band") * lax.axis_size("sector")
    return lax.ppermute(array, ("band", "sector"), [(i, i ^ mask) for i in range(count)])


def position():
    return lax.axis_index("band") * lax.axis_size("sector") + lax.axis_index("sector")


def quarter(array, index):
    rows = array.shape[0] // 4
    return lax.dynamic_slice_in_dim(array, index * rows, rows, 0)


def plus(first, *others):
    total = first.astype(F32)
    for other in others:
        total = total + other.astype(F32)
    return total.astype(BF16)


def summed_halves(array, beside_first, beside_second):
    count = lax.axis_size("band") * lax.axis_size("sector")
    here = position()
    half = array.shape[0] // 2
    bit = here % 2
    give = lax.dynamic_slice_in_dim(array, (1 - bit) * half, half, 0)
    keep = lax.dynamic_slice_in_dim(array, bit * half, half, 0)
    held = plus(keep, flipped(give, 1))
    place = (here // 2) % 4
    got = [flipped(quarter(held, place ^ turn), 2 * turn) for turn in (3, 1, 2)]
    part = plus(quarter(held, place), *got)
    part, first = lax.optimization_barrier((part, beside_first()))
    second = beside_second(first)
    masks, step = [], 8
    while step < count:
        masks.append(step)
        step *= 2
    if len(masks) > 1:
        masks[1] |= masks[0]
    for mask in masks:
        part = plus(part, flipped(part, mask))
    part, second = lax.optimization_barrier((part, second))
    parts = {turn: flipped(part, 2 * turn) for turn in (3, 1, 2)}
    parts[0] = part
    rows = []
    for at in range(4):
        chosen = parts[at ^ 3]
        for turn in range(3):
            chosen = jnp.where(place == turn, parts[at ^ turn], chosen)
        rows.append(chosen)
    held = jnp.concatenate(rows)
    return held, flipped(held, 1), second


def dot(a, b, ca=1, cb=0):
    return lax.dot_general(a, b, (((ca,), (cb,)), ((), ())), preferred_element_type=F32)


def doubled(values):
    return jnp.concatenate([values, values], axis=1)


def row_mean(values):
    return jnp.mean(values, axis=-1, keepdims=True)


def silu_parts(v):
    gate = 0.5 * jnp.tanh(0.5 * v) + 0.5
    out = v * gate
    return out, gate + out * (1.0 - gate)


def picked(rows, count):
    flat = jnp.concatenate([rows[j : j + 1, :] for j in range(rows.shape[0])], axis=1)
    lines = lax.broadcasted_iota(jnp.int32, (count, flat.shape[1]), 0)
    return jnp.where(flat == lines, 1.0, 0.0).astype(BF16)


def provide_kernel(rows_hbm, node_hbm, w_hbm, ahead_ref, behind_ref, same_ref, own_ref, w_ref, rows_ref, sem):
    copies = [
        pltpu.make_async_copy(src, dst, sem.at[place])
        for place, (src, dst) in enumerate(
            ((rows_hbm, rows_ref), (node_hbm, own_ref), (w_hbm, w_ref))
        )
    ]
    for copy in copies:
        copy.start()
    copies[0].wait()
    pick = picked(rows_ref[...], own_ref.shape[0])
    copies[1].wait()
    rows = dot(pick, own_ref[...], 0, 0).astype(BF16)
    cap = rows_ref.shape[1]
    for ref, members in ((ahead_ref, AHEAD), (behind_ref, BEHIND), (same_ref, SAME)):
        for place, course in enumerate(members):
            ref[place * cap : (place + 1) * cap, :] = rows[course * cap : (course + 1) * cap, :]
    copies[2].wait()


def collect_kernel(rows_ref, ahead_ref, behind_ref, same_ref, partial_ref, w_ref, out_ref):
    cap = rows_ref.shape[1]
    pieces = {}
    for ref, members in ((ahead_ref, AHEAD), (behind_ref, BEHIND), (same_ref, SAME)):
        for place, course in enumerate(members):
            pieces[course] = ref[place * cap : (place + 1) * cap, :]
    arrived = jnp.concatenate([pieces[course] for course in range(8)])
    total = dot(picked(rows_ref[...], partial_ref.shape[0]), arrived).astype(BF16)
    out_ref[...] = partial_ref[...] + dot(total, w_ref[...], 1, 1)


def finish_kernel(bit_ref, held_ref, got_ref, in_ref, out_ref, node_in_ref, node_out_ref, *, scale):
    first = bit_ref[0] == 0
    held = held_ref[...].astype(F32) * scale
    got = got_ref[...].astype(F32) * scale
    halves = (jnp.where(first, held, got), jnp.where(first, got, held))
    half = held.shape[0]
    start = 0
    for ref in (in_ref, out_ref, node_in_ref, node_out_ref):
        rows = ref.shape[0]
        for side in range(2):
            lo, hi = max(start, side * half), min(start + rows, (side + 1) * half)
            if lo < hi:
                ref[lo - start : hi - start, :] = halves[side][lo - side * half : hi - side * half, :]
        start += rows


def pieces_of(chunk):
    def piece(index):
        return pl.ds(pl.multiple_of(index * chunk, chunk), chunk)

    return piece


def one_hot(values, lanes, first, last):
    parts = [jnp.where(values == lanes + at, 1.0, 0.0).astype(BF16) for at in range(first, last, 128)]
    return jnp.concatenate(parts, axis=1)


class Wide:
    def __init__(self, ref, slots):
        self.ref, self.slots = ref, slots
        self.blocks, self.rows = ref.shape[0], ref.shape[1] // slots

    def spread(self, rows):
        for k in range(self.slots):
            for block in range(self.blocks):
                part = rows[:, block * 128 : (block + 1) * 128]
                self.ref[block, pl.ds(k, self.rows, stride=self.slots), :] = part

    def get(self):
        return jnp.concatenate([self.ref[block] for block in range(self.blocks)], axis=1)

    def put(self, values):
        for block in range(self.blocks):
            self.ref[block] = values[:, block * 128 : (block + 1) * 128]

    def folded(self):
        parts = []
        for block in range(self.blocks):
            total = self.ref[block, pl.ds(0, self.rows, stride=self.slots), :]
            for k in range(1, self.slots):
                total = total + self.ref[block, pl.ds(k, self.rows, stride=self.slots), :]
            parts.append(total)
        return jnp.concatenate(parts, axis=1)


def near_kernel(
    slot_ref,
    mask_ref,
    b_edge_ref,
    after_ref,
    own_ref,
    w_in_ref,
    edge_hbm,
    w_out_hbm,
    wn_in_hbm,
    wn_out_hbm,
    node_cot_hbm,
    near_ref,
    code_ref,
    edge_ref,
    w_out_ref,
    wn_in_ref,
    wn_out_ref,
    node_cot_ref,
    proj_v,
    recv_v,
    wide_v,
    sem_in,
    sem_whole,
    *,
    chunk,
):
    nodes, d = own_ref.shape
    edges = edge_ref.shape[0]
    slots = edges // nodes
    count = edges // chunk
    cn = chunk // slots
    piece = pieces_of(chunk)

    def pull(index):
        return pltpu.make_async_copy(edge_hbm.at[piece(index)], edge_ref.at[piece(index)], sem_in.at[index])

    wholes = [
        pltpu.make_async_copy(src, dst, sem_whole.at[place])
        for place, (src, dst) in enumerate(
            (
                (w_out_hbm, w_out_ref),
                (wn_in_hbm, wn_in_ref),
                (wn_out_hbm, wn_out_ref),
                (node_cot_hbm, node_cot_ref),
            )
        )
    ]
    for index in range(count):
        pull(index).start()
    for copy in wholes:
        copy.start()
    code = slot_ref[...] * 2 + mask_ref[...]
    for k in range(slots):
        code_ref[pl.ds(k, nodes, stride=slots), :] = jnp.broadcast_to(code[:, k : k + 1], (nodes, 128))
    own = own_ref[...]
    proj_v[...] = dot(own, w_in_ref[d : 2 * d, :]).astype(BF16)
    recv_v[...] = dot(own, w_in_ref[2 * d :, :]) + b_edge_ref[...]
    lanes = lax.broadcasted_iota(jnp.int32, (chunk, 128), 1)
    wide = Wide(wide_v, slots)

    def step(index, carry):
        rows = piece(index)
        pull(index).wait()
        wide.spread(recv_v[pl.ds(pl.multiple_of(index * cn, cn), cn), :])
        pick = one_hot(lax.shift_right_logical(code_ref[rows, :], 1), lanes, 0, nodes)
        near_ref[rows, :] = 0.5 * (dot(edge_ref[rows, :], w_in_ref[:d, :]) + dot(pick, proj_v[...]) + wide.get())
        return carry

    lax.fori_loop(0, count, step, 0)
    for copy in wholes:
        copy.wait()


def layer_kernel(
    slot_row_ref,
    g_edge_ref,
    b_node_ref,
    g_node_ref,
    up_ref,
    down_ref,
    ahead_ref,
    behind_ref,
    own_ref,
    w_in_ref,
    near_v,
    code_v,
    edge_v,
    w_out_ref,
    wn_in_ref,
    wn_out_ref,
    node_cot_v,
    cot_hbm,
    node_new_ref,
    new_hbm,
    partial_ref,
    grad_hbm,
    up_back_ref,
    down_back_ref,
    level_back_ref,
    wg_ref,
    cot_v,
    new_v,
    grad_v,
    hid_v,
    slope_v,
    norm_v,
    scale_v,
    table_v,
    proj_v,
    gath_v,
    dgath_v,
    drecv_v,
    wide_v,
    t_acc,
    we_acc,
    wo_acc,
    back_v,
    dy_v,
    dpre_v,
    sem_in,
    sem_out,
    *,
    chunk,
):
    nodes, d = own_ref.shape
    edges = edge_v.shape[0]
    slots = edges // nodes
    cap = up_ref.shape[0] // 3
    table = nodes + 8 * cap
    count = edges // chunk
    cn = chunk // slots
    piece = pieces_of(chunk)

    def pull(index):
        return pltpu.make_async_copy(cot_hbm.at[piece(index)], cot_v.at[piece(index)], sem_in.at[index])

    def push(kind, index):
        src, dst = ((new_v, new_hbm), (grad_v, grad_hbm))[kind]
        return pltpu.make_async_copy(src.at[piece(index)], dst.at[piece(index)], sem_out.at[kind, index])

    for index in range(count):
        pull(index).start()

    level = (behind_ref[cap : 2 * cap, :], ahead_ref[cap : 2 * cap, :])
    for members, rows in ((UP, up_ref[...]), (DOWN, down_ref[...]), (LEVEL, jnp.concatenate(level))):
        for place, course in enumerate(members):
            at = nodes + course * cap
            table_v[at : at + cap, :] = rows[place * cap : (place + 1) * cap, :]
    proj_v[...] = (0.5 * dot(table_v[nodes:, :], w_in_ref[d : 2 * d, :])).astype(BF16)
    back_v[...] = 0.5 * w_out_ref[...]
    gain = g_edge_ref[...]
    lanes = lax.broadcasted_iota(jnp.int32, (chunk, 128), 1)
    wides = (Wide(wide_v.at[0], slots), Wide(wide_v.at[1], slots))
    wide = wides[0]

    def part(index):
        return pl.ds(pl.multiple_of(index * cn, cn), cn)

    def open_lead(index, side):
        rows = piece(index)
        pick = one_hot(lax.shift_right_logical(code_v[rows, :], 1), lanes, nodes, table)
        half = near_v[rows, :] + dot(pick, proj_v[...])
        bend = jnp.tanh(half)
        gate = bend + 1.0
        hidden = half * gate
        slope_v[rows, :] = (gate + hidden * (1.0 - bend)).astype(BF16)
        hidden = hidden.astype(BF16)
        hid_v[rows, :] = hidden
        dy_v[side] = hidden

    def open_trail(index, side):
        rows = piece(index)
        buffer = wides[side]
        y = dot(dy_v[side], w_out_ref[...])
        y = y - row_mean(y)
        rstd = lax.rsqrt(row_mean(y * y) + 1e-05)
        scale = (code_v[rows, :] & 1).astype(F32) * rstd
        scale_v[rows, :] = scale
        norm = y * doubled(scale)
        norm_v[rows, :] = norm.astype(BF16)
        update = norm * gain
        new_v[rows, :] = (edge_v[rows, :].astype(F32) + update).astype(BF16)
        buffer.put(update)
        gath_v[part(index), :] = buffer.folded().astype(BF16)

    open_lead(0, 0)

    def ahead(pair, carry):
        open_trail(2 * pair, 0)
        open_lead(2 * pair + 1, 1)
        push(0, 2 * pair).start()
        open_trail(2 * pair + 1, 1)
        open_lead(2 * pair + 2, 0)
        push(0, 2 * pair + 1).start()
        return carry

    lax.fori_loop(0, count // 2 - 1, ahead, 0)
    open_trail(count - 2, 0)
    open_lead(count - 1, 1)
    open_trail(count - 1, 1)
    push(0, count - 2).start()
    push(0, count - 1).start()

    own = own_ref[...]
    table_v[:nodes, :] = own
    gathered = gath_v[...]
    pre = dot(own, wn_in_ref[:d, :]) + dot(gathered, wn_in_ref[d:, :]) + b_node_ref[...]
    hidden, slope = silu_parts(pre)
    hidden = hidden.astype(BF16)
    y = dot(hidden, wn_out_ref[...])
    y = y - row_mean(y)
    rstd = lax.rsqrt(row_mean(y * y) + 1e-05)
    norm = y * rstd
    node_new_ref[...] = (own.astype(F32) + norm * g_node_ref[...]).astype(BF16)
    node_cot = node_cot_v[...].astype(F32)
    a = node_cot * g_node_ref[...]
    dy = ((a - row_mean(a) - norm * row_mean(a * norm)) * rstd).astype(BF16)
    dpre = (dot(dy, wn_out_ref[...], 1, 1) * slope).astype(BF16)
    dgath_v[...] = dot(dpre, wn_in_ref[d:, :], 1, 1)
    partial_ref[...] = node_cot + dot(dpre, wn_in_ref[:d, :], 1, 1)
    wg_ref[4 * d : 5 * d, :] = dot(own, dpre, 0, 0).astype(BF16)
    wg_ref[5 * d : 6 * d, :] = dot(gathered, dpre, 0, 0).astype(BF16)
    wg_ref[6 * d : 7 * d, :] = dot(hidden, dy, 0, 0).astype(BF16)

    t_acc[...] = jnp.zeros_like(t_acc)
    we_acc[...] = jnp.zeros_like(we_acc)
    wo_acc[...] = jnp.zeros_like(wo_acc)
    lines = lax.broadcasted_iota(jnp.int32, (table, chunk), 0)

    def lead(index, side):
        rows = piece(index)
        cot = cot_v[rows, :].astype(F32)
        buffer = wides[side]
        buffer.spread(dgath_v[part(index), :])
        a = (cot + buffer.get()) * gain
        norm = norm_v[rows, :].astype(F32)
        dy = ((a - row_mean(a) - norm * row_mean(a * norm)) * doubled(scale_v[rows, :])).astype(BF16)
        dpre = dot(dy, back_v[...], 1, 1) * slope_v[rows, :].astype(F32)
        buffer.put(dpre)
        drecv_v[part(index), :] = buffer.folded().astype(BF16)
        dy_v[side] = dy
        dpre_v[side] = dpre.astype(BF16)

    def trail(index, side):
        rows = piece(index)
        dy, dpre = dy_v[side], dpre_v[side]
        grad_v[rows, :] = (cot_v[rows, :].astype(F32) + dot(dpre, w_in_ref[:d, :], 1, 1)).astype(BF16)
        wo_acc[...] += dot(hid_v[rows, :], dy, 0, 0)
        we_acc[...] += dot(edge_v[rows, :], dpre, 0, 0)
        pick = jnp.where(slot_row_ref[:, rows] == lines, 1.0, 0.0).astype(BF16)
        t_acc[...] += dot(pick, dpre)

    for index in range(count):
        pull(index).wait()
    lead(0, 0)

    def behind(pair, carry):
        trail(2 * pair, 0)
        lead(2 * pair + 1, 1)
        push(1, 2 * pair).start()
        trail(2 * pair + 1, 1)
        lead(2 * pair + 2, 0)
        push(1, 2 * pair + 1).start()
        return carry

    lax.fori_loop(0, count // 2 - 1, behind, 0)
    trail(count - 2, 0)
    lead(count - 1, 1)
    trail(count - 1, 1)
    push(1, count - 2).start()
    push(1, count - 1).start()

    total = t_acc[...].astype(BF16)
    for members, ref in ((UP, up_back_ref), (DOWN, down_back_ref), (LEVEL, level_back_ref)):
        for place, course in enumerate(members):
            at = nodes + course * cap
            ref[place * cap : (place + 1) * cap, :] = total[at : at + cap, :]
    drecv = drecv_v[...]
    partial_ref[...] += dot(total[:nodes, :], w_in_ref[d : 2 * d, :], 1, 1) + dot(drecv, w_in_ref[2 * d :, :], 1, 1)
    wg_ref[:d, :] = we_acc[...].astype(BF16)
    wg_ref[d : 2 * d, :] = dot(table_v[...], total, 0, 0).astype(BF16)
    wg_ref[2 * d : 3 * d, :] = dot(own, drecv, 0, 0).astype(BF16)
    wg_ref[3 * d : 4 * d, :] = wo_acc[...].astype(BF16)
    for kind in range(2):
        for index in range(count):
            push(kind, index).wait()


def local(
    node_latent,
    edge_latent,
    sender_slot,
    edge_mask,
    send_rows,
    w_edge_in,
    b_edge,
    w_edge_out,
    g_edge,
    w_node_in,
    b_node,
    w_node_out,
    g_node,
    node_cot,
    edge_cot,
):
    nodes, d = node_latent.shape
    edges = edge_latent.shape[0]
    slots = sender_slot.shape[1]
    capacity = send_rows.shape[2]
    far = 8 * capacity
    table = nodes + far
    devices = lax.axis_size("band") * lax.axis_size("sector")
    params = pltpu.CompilerParams(vmem_limit_bytes=34 * 1024 * 1024)
    shape = jax.ShapeDtypeStruct
    rows = send_rows.reshape(8, capacity)
    vmem = pl.BlockSpec(memory_space=pltpu.VMEM)
    hbm = pl.BlockSpec(memory_space=pltpu.HBM)
    free = pl.BlockSpec(memory_space=pl.ANY)
    dma = pltpu.SemaphoreType.DMA

    def off_chip(array):
        return pltpu.with_memory_space_constraint(array, pltpu.HBM)

    def on_chip(array):
        return pltpu.with_memory_space_constraint(array, pltpu.VMEM)

    w_shape = w_edge_in.shape
    ahead, behind, same, own, w_in = pl.pallas_call(
        provide_kernel,
        in_specs=[hbm] * 3,
        out_specs=(vmem,) * 5,
        out_shape=tuple(pltpu.VMEM((len(m) * capacity, d), BF16) for m in (AHEAD, BEHIND, SAME))
        + (pltpu.VMEM((nodes, d), BF16), pltpu.VMEM(w_shape, BF16)),
        scratch_shapes=[pltpu.VMEM(rows.shape, rows.dtype), dma((3,))],
        compiler_params=params,
    )(off_chip(rows), off_chip(node_latent), off_chip(w_edge_in))

    def course_of(course, sets):
        for members, block in sets:
            if course in members:
                at = members.index(course) * capacity
                return block[at : at + capacity]

    def gathered_rows(courses, sets):
        return jnp.concatenate([course_of(course, sets) for course in courses])

    ahead, behind = shifted(ahead, "sector", -1), shifted(behind, "sector", 1)
    sets = ((AHEAD, ahead), (BEHIND, behind), (SAME, same))
    up = shifted(gathered_rows(UP, sets), "band", -1)
    down = shifted(gathered_rows(DOWN, sets), "band", 1)

    chunk = 64 * slots
    count = edges // chunk
    near, code, edge, w_out, wn_in, wn_out, node_cot_near = pl.pallas_call(
        functools.partial(near_kernel, chunk=chunk),
        out_shape=(pltpu.VMEM((edges, d), F32), pltpu.VMEM((edges, 128), jnp.int32), pltpu.VMEM((edges, d), BF16))
        + tuple(pltpu.VMEM(x.shape, BF16) for x in (w_edge_out, w_node_in, w_node_out, node_cot)),
        in_specs=[vmem] * 3 + [free] + [vmem] * 2 + [hbm] * 5,
        out_specs=(vmem,) * 7,
        scratch_shapes=[
            pltpu.VMEM((nodes, d), BF16),
            pltpu.VMEM((nodes, d), F32),
            pltpu.VMEM((d // 128, chunk, 128), F32),
            dma((count,)),
            dma((4,)),
        ],
        compiler_params=params,
        cost_estimate=pl.CostEstimate(flops=6 * edges * d * d, transcendentals=0, bytes_accessed=16 * edges * d),
    )(
        sender_slot,
        edge_mask,
        b_edge.reshape(1, d),
        ahead,
        on_chip(own),
        on_chip(w_in),
        off_chip(edge_latent),
        off_chip(w_edge_out),
        off_chip(w_node_in),
        off_chip(w_node_out),
        off_chip(node_cot),
    )
    node_new, edge_new, partial, edge_grad, up_back, down_back, level_back, grads = pl.pallas_call(
        functools.partial(layer_kernel, chunk=chunk),
        out_shape=(
            shape((nodes, d), BF16),
            shape((edges, d), BF16),
            pltpu.VMEM((nodes, d), F32),
            shape((edges, d), BF16),
            pltpu.VMEM((3 * capacity, d), BF16),
            pltpu.VMEM((3 * capacity, d), BF16),
            pltpu.VMEM((2 * capacity, d), BF16),
            pltpu.VMEM((7 * d, d), BF16),
        ),
        in_specs=[vmem] * 17 + [hbm],
        out_specs=(vmem, hbm, vmem, hbm, vmem, vmem, vmem, vmem),
        scratch_shapes=[
            pltpu.VMEM((edges, d), BF16),
            pltpu.VMEM((edges, d), BF16),
            pltpu.VMEM((edges, d), BF16),
            pltpu.VMEM((edges, d), BF16),
            pltpu.VMEM((edges, d), BF16),
            pltpu.VMEM((edges, d), BF16),
            pltpu.VMEM((edges, 128), F32),
            pltpu.VMEM((table, d), BF16),
            pltpu.VMEM((far, d), BF16),
            pltpu.VMEM((nodes, d), BF16),
            pltpu.VMEM((nodes, d), F32),
            pltpu.VMEM((nodes, d), BF16),
            pltpu.VMEM((2, d // 128, chunk, 128), F32),
            pltpu.VMEM((table, d), F32),
            pltpu.VMEM((d, d), F32),
            pltpu.VMEM((d, d), F32),
            pltpu.VMEM((d, d), BF16),
            pltpu.VMEM((2, chunk, d), BF16),
            pltpu.VMEM((2, chunk, d), BF16),
            dma((count,)),
            dma((2, count)),
        ],
        compiler_params=params,
    )(
        sender_slot.reshape(1, edges),
        g_edge.reshape(1, d),
        b_node.reshape(1, d),
        g_node.reshape(1, d),
        up,
        down,
        ahead,
        behind,
        on_chip(own),
        on_chip(w_in),
        on_chip(near),
        on_chip(code),
        on_chip(edge),
        on_chip(w_out),
        on_chip(wn_in),
        on_chip(wn_out),
        on_chip(node_cot_near),
        off_chip(edge_cot),
    )

    def return_bands():
        return shifted(up_back, "band", 1), shifted(down_back, "band", -1)

    def return_sectors(moved):
        sets = ((UP, moved[0]), (DOWN, moved[1]), (LEVEL, level_back))
        ahead = shifted(gathered_rows(AHEAD, sets), "sector", 1)
        behind = shifted(gathered_rows(BEHIND, sets), "sector", -1)
        return ahead, behind, gathered_rows(SAME, sets)

    held, got, (ahead, behind, same) = summed_halves(grads, return_bands, return_sectors)
    whole = lambda *dims: pl.BlockSpec(dims, lambda i: (0,) * len(dims))
    node_grad = pl.pallas_call(
        collect_kernel,
        grid=(1,),
        in_specs=[
            whole(8, capacity),
            whole(3 * capacity, d),
            whole(3 * capacity, d),
            whole(2 * capacity, d),
            whole(nodes, d),
            pl.BlockSpec((d, d), lambda i: (1, 0)),
        ],
        out_specs=whole(nodes, d),
        out_shape=shape((nodes, d), F32),
        compiler_params=params,
    )(rows, ahead, behind, same, partial, w_in)
    grad_in, grad_out, grad_node_in, grad_node_out = pl.pallas_call(
        functools.partial(finish_kernel, scale=float(devices * edges) ** (-0.5)),
        in_specs=[pl.BlockSpec(memory_space=pltpu.SMEM), vmem, vmem],
        out_specs=(vmem,) * 4,
        out_shape=tuple(shape((parts * d, d), F32) for parts in (3, 1, 2, 1)),
        compiler_params=params,
    )((position() % 2).reshape(1), held, got)
    return (node_new, edge_new, node_grad, edge_grad, grad_in, grad_out, grad_node_in, grad_node_out)


def solution(mesh):
    split = P(("band", "sector"), None)
    in_specs = (split, split, split, split, P(("band", "sector"), None, None))
    in_specs += (P(),) * 8 + (split, split)
    out_specs = (split,) * 4 + (P(),) * 4
    return jax.shard_map(local, mesh=mesh, in_specs=in_specs, out_specs=out_specs, check_vma=False)
```

```python
import functools

import jax
import jax.numpy as jnp
from jax import lax
from jax.experimental import pallas as pl
from jax.experimental.pallas import tpu as pltpu
from jax.sharding import PartitionSpec as P

band_steps = (-1, -1, -1, 0, 0, 1, 1, 1)
sector_steps = (-1, 0, 1, -1, 1, -1, 0, 1)
AHEAD = tuple(j for j in range(8) if sector_steps[j] == 1)
BEHIND = tuple(j for j in range(8) if sector_steps[j] == -1)
SAME = tuple(j for j in range(8) if sector_steps[j] == 0)
UP = tuple(j for j in range(8) if band_steps[j] == 1)
DOWN = tuple(j for j in range(8) if band_steps[j] == -1)
LEVEL = tuple(j for j in range(8) if band_steps[j] == 0)
BF16 = jnp.bfloat16
F32 = jnp.float32


def shifted(array, axis, by):
    count = lax.axis_size(axis)
    return lax.ppermute(array, axis, [(i, (i + by) % count) for i in range(count)])


def over_bands(up, down):
    count = lax.axis_size("band")
    if count % 2:
        return shifted(up, "band", -1), shifted(down, "band", 1)
    even = lax.axis_index("band") % 2 == 0
    near = [(i, i ^ 1) for i in range(count)]
    cross = [(i, i if i in (0, count - 1) else i + 1 if i % 2 else i - 1) for i in range(count)]
    first = lax.ppermute(jnp.where(even, down, up), "band", near)
    second = lax.ppermute(jnp.where(even, up, down), "band", cross)
    return jnp.where(even, first, second), jnp.where(even, second, first)


def flipped(array, mask):
    count = lax.axis_size("band") * lax.axis_size("sector")
    return lax.ppermute(array, ("band", "sector"), [(i, i ^ mask) for i in range(count)])


def position():
    return lax.axis_index("band") * lax.axis_size("sector") + lax.axis_index("sector")


def quarter(array, index):
    rows = array.shape[0] // 4
    return lax.dynamic_slice_in_dim(array, index * rows, rows, 0)


def plus(first, *others):
    total = first.astype(F32)
    for other in others:
        total = total + other.astype(F32)
    return total.astype(BF16)


def summed_halves(array, beside_first, beside_second):
    count = lax.axis_size("band") * lax.axis_size("sector")
    here = position()
    half = array.shape[0] // 2
    bit = here % 2
    give = lax.dynamic_slice_in_dim(array, (1 - bit) * half, half, 0)
    keep = lax.dynamic_slice_in_dim(array, bit * half, half, 0)
    held = plus(keep, flipped(give, 1))
    place = (here // 2) % 4
    got = [flipped(quarter(held, place ^ turn), 2 * turn) for turn in (3, 1, 2)]
    part = plus(quarter(held, place), *got)
    part, first = lax.optimization_barrier((part, beside_first()))
    second = beside_second(first)
    masks, step = [], 8
    while step < count:
        masks.append(step)
        step *= 2
    if len(masks) > 1:
        masks[1] |= masks[0]
    for mask in masks:
        part = plus(part, flipped(part, mask))
    parts = {turn: flipped(part, 2 * turn) for turn in (3, 1, 2)}
    parts[0] = part
    rows = []
    for at in range(4):
        chosen = parts[at ^ 3]
        for turn in range(3):
            chosen = jnp.where(place == turn, parts[at ^ turn], chosen)
        rows.append(chosen)
    held, second = lax.optimization_barrier((jnp.concatenate(rows), second))
    return held, flipped(held, 1), second


def dot(a, b, ca=1, cb=0):
    return lax.dot_general(a, b, (((ca,), (cb,)), ((), ())), preferred_element_type=F32)


def doubled(values):
    return jnp.concatenate([values, values], axis=1)


def row_mean(values):
    return jnp.mean(values, axis=-1, keepdims=True)


def silu_parts(v):
    gate = 0.5 * jnp.tanh(0.5 * v) + 0.5
    out = v * gate
    return out, gate + out * (1.0 - gate)


def picked(rows, count):
    flat = jnp.concatenate([rows[j : j + 1, :] for j in range(rows.shape[0])], axis=1)
    lines = lax.broadcasted_iota(jnp.int32, (count, flat.shape[1]), 0)
    return jnp.where(flat == lines, 1.0, 0.0).astype(BF16)


def provide_kernel(rows_hbm, node_hbm, w_hbm, ahead_ref, behind_ref, same_ref, own_ref, w_ref, rows_ref, sem):
    copies = [
        pltpu.make_async_copy(src, dst, sem.at[place])
        for place, (src, dst) in enumerate(
            ((rows_hbm, rows_ref), (node_hbm, own_ref), (w_hbm, w_ref))
        )
    ]
    for copy in copies:
        copy.start()
    copies[0].wait()
    pick = picked(rows_ref[...], own_ref.shape[0])
    copies[1].wait()
    rows = dot(pick, own_ref[...], 0, 0).astype(BF16)
    cap = rows_ref.shape[1]
    for ref, members in ((ahead_ref, AHEAD), (behind_ref, BEHIND), (same_ref, SAME)):
        for place, course in enumerate(members):
            ref[place * cap : (place + 1) * cap, :] = rows[course * cap : (course + 1) * cap, :]
    copies[2].wait()


def collect_kernel(rows_ref, up_ref, down_ref, level_ref, partial_ref, w_ref, out_ref):
    cap = rows_ref.shape[1]
    pieces = {}
    for ref, members in ((up_ref, UP), (down_ref, DOWN), (level_ref, LEVEL)):
        for place, course in enumerate(members):
            pieces[course] = ref[place * cap : (place + 1) * cap, :]
    arrived = jnp.concatenate([pieces[course] for course in range(8)])
    total = dot(picked(rows_ref[...], partial_ref.shape[0]), arrived).astype(BF16)
    out_ref[...] = partial_ref[...] + dot(total, w_ref[...], 1, 1)


def finish_kernel(bit_ref, held_ref, got_ref, in_ref, out_ref, node_in_ref, node_out_ref, *, scale):
    first = bit_ref[0] == 0
    held = held_ref[...].astype(F32) * scale
    got = got_ref[...].astype(F32) * scale
    halves = (jnp.where(first, held, got), jnp.where(first, got, held))
    half = held.shape[0]
    start = 0
    for ref in (in_ref, out_ref, node_in_ref, node_out_ref):
        rows = ref.shape[0]
        for side in range(2):
            lo, hi = max(start, side * half), min(start + rows, (side + 1) * half)
            if lo < hi:
                ref[lo - start : hi - start, :] = halves[side][lo - side * half : hi - side * half, :]
        start += rows


def pieces_of(chunk):
    def piece(index):
        return pl.ds(pl.multiple_of(index * chunk, chunk), chunk)

    return piece


def one_hot(values, lanes, first, last):
    parts = [jnp.where(values == lanes + at, 1.0, 0.0).astype(BF16) for at in range(first, last, 128)]
    return jnp.concatenate(parts, axis=1)


class Wide:
    def __init__(self, ref, slots):
        self.ref, self.slots = ref, slots
        self.blocks, self.rows = ref.shape[0], ref.shape[1] // slots

    def spread(self, rows):
        for k in range(self.slots):
            for block in range(self.blocks):
                part = rows[:, block * 128 : (block + 1) * 128]
                self.ref[block, pl.ds(k, self.rows, stride=self.slots), :] = part

    def get(self):
        return jnp.concatenate([self.ref[block] for block in range(self.blocks)], axis=1)

    def put(self, values):
        for block in range(self.blocks):
            self.ref[block] = values[:, block * 128 : (block + 1) * 128]

    def folded(self):
        parts = []
        for block in range(self.blocks):
            total = self.ref[block, pl.ds(0, self.rows, stride=self.slots), :]
            for k in range(1, self.slots):
                total = total + self.ref[block, pl.ds(k, self.rows, stride=self.slots), :]
            parts.append(total)
        return jnp.concatenate(parts, axis=1)


def near_kernel(
    slot_ref,
    mask_ref,
    b_edge_ref,
    after_ref,
    own_ref,
    w_in_ref,
    edge_hbm,
    w_out_hbm,
    wn_in_hbm,
    wn_out_hbm,
    node_cot_hbm,
    near_ref,
    code_ref,
    edge_ref,
    w_out_ref,
    wn_in_ref,
    wn_out_ref,
    node_cot_ref,
    proj_v,
    recv_v,
    wide_v,
    sem_in,
    sem_whole,
    *,
    chunk,
):
    nodes, d = own_ref.shape
    edges = edge_ref.shape[0]
    slots = edges // nodes
    count = edges // chunk
    cn = chunk // slots
    piece = pieces_of(chunk)

    def pull(index):
        return pltpu.make_async_copy(edge_hbm.at[piece(index)], edge_ref.at[piece(index)], sem_in.at[index])

    wholes = [
        pltpu.make_async_copy(src, dst, sem_whole.at[place])
        for place, (src, dst) in enumerate(
            (
                (w_out_hbm, w_out_ref),
                (wn_in_hbm, wn_in_ref),
                (wn_out_hbm, wn_out_ref),
                (node_cot_hbm, node_cot_ref),
            )
        )
    ]
    for index in range(count):
        pull(index).start()
    for copy in wholes:
        copy.start()
    code = slot_ref[...] * 2 + mask_ref[...]
    for k in range(slots):
        code_ref[pl.ds(k, nodes, stride=slots), :] = jnp.broadcast_to(code[:, k : k + 1], (nodes, 128))
    own = own_ref[...]
    proj_v[...] = dot(own, w_in_ref[d : 2 * d, :]).astype(BF16)
    recv_v[...] = dot(own, w_in_ref[2 * d :, :]) + b_edge_ref[...]
    lanes = lax.broadcasted_iota(jnp.int32, (chunk, 128), 1)
    wide = Wide(wide_v, slots)

    def step(index, carry):
        rows = piece(index)
        pull(index).wait()
        wide.spread(recv_v[pl.ds(pl.multiple_of(index * cn, cn), cn), :])
        pick = one_hot(lax.shift_right_logical(code_ref[rows, :], 1), lanes, 0, nodes)
        near_ref[rows, :] = 0.5 * (dot(edge_ref[rows, :], w_in_ref[:d, :]) + dot(pick, proj_v[...]) + wide.get())
        return carry

    lax.fori_loop(0, count, step, 0)
    for copy in wholes:
        copy.wait()


def layer_kernel(
    slot_row_ref,
    g_edge_ref,
    b_node_ref,
    g_node_ref,
    up_ref,
    down_ref,
    ahead_ref,
    behind_ref,
    own_ref,
    w_in_ref,
    near_v,
    code_v,
    edge_v,
    w_out_ref,
    wn_in_ref,
    wn_out_ref,
    node_cot_v,
    cot_hbm,
    node_new_ref,
    new_hbm,
    partial_ref,
    grad_hbm,
    ahead_back_ref,
    behind_back_ref,
    same_back_ref,
    wg_ref,
    cot_v,
    new_v,
    grad_v,
    hid_v,
    slope_v,
    norm_v,
    scale_v,
    table_v,
    proj_v,
    gath_v,
    dgath_v,
    drecv_v,
    wide_v,
    t_acc,
    we_acc,
    wo_acc,
    back_v,
    dy_v,
    dpre_v,
    sem_in,
    sem_out,
    *,
    chunk,
):
    nodes, d = own_ref.shape
    edges = edge_v.shape[0]
    slots = edges // nodes
    cap = up_ref.shape[0] // 3
    table = nodes + 8 * cap
    count = edges // chunk
    cn = chunk // slots
    piece = pieces_of(chunk)

    def pull(index):
        return pltpu.make_async_copy(cot_hbm.at[piece(index)], cot_v.at[piece(index)], sem_in.at[index])

    def push(kind, index):
        src, dst = ((new_v, new_hbm), (grad_v, grad_hbm))[kind]
        return pltpu.make_async_copy(src.at[piece(index)], dst.at[piece(index)], sem_out.at[kind, index])

    for index in range(count):
        pull(index).start()

    level = (behind_ref[cap : 2 * cap, :], ahead_ref[cap : 2 * cap, :])
    for members, rows in ((UP, up_ref[...]), (DOWN, down_ref[...]), (LEVEL, jnp.concatenate(level))):
        for place, course in enumerate(members):
            at = nodes + course * cap
            table_v[at : at + cap, :] = rows[place * cap : (place + 1) * cap, :]
    proj_v[...] = (0.5 * dot(table_v[nodes:, :], w_in_ref[d : 2 * d, :])).astype(BF16)
    back_v[...] = 0.5 * w_out_ref[...]
    gain = g_edge_ref[...]
    lanes = lax.broadcasted_iota(jnp.int32, (chunk, 128), 1)
    wides = (Wide(wide_v.at[0], slots), Wide(wide_v.at[1], slots))
    wide = wides[0]

    def part(index):
        return pl.ds(pl.multiple_of(index * cn, cn), cn)

    def open_lead(index, side):
        rows = piece(index)
        pick = one_hot(lax.shift_right_logical(code_v[rows, :], 1), lanes, nodes, table)
        half = near_v[rows, :] + dot(pick, proj_v[...])
        bend = jnp.tanh(half)
        gate = bend + 1.0
        hidden = half * gate
        slope_v[rows, :] = (gate + hidden * (1.0 - bend)).astype(BF16)
        hidden = hidden.astype(BF16)
        hid_v[rows, :] = hidden
        dy_v[side] = hidden

    def open_trail(index, side):
        rows = piece(index)
        buffer = wides[side]
        y = dot(dy_v[side], w_out_ref[...])
        y = y - row_mean(y)
        rstd = lax.rsqrt(row_mean(y * y) + 1e-05)
        scale = (code_v[rows, :] & 1).astype(F32) * rstd
        scale_v[rows, :] = scale
        norm = y * doubled(scale)
        norm_v[rows, :] = norm.astype(BF16)
        update = norm * gain
        new_v[rows, :] = (edge_v[rows, :].astype(F32) + update).astype(BF16)
        buffer.put(update)
        gath_v[part(index), :] = buffer.folded().astype(BF16)

    open_lead(0, 0)

    def ahead(pair, carry):
        open_trail(2 * pair, 0)
        open_lead(2 * pair + 1, 1)
        push(0, 2 * pair).start()
        open_trail(2 * pair + 1, 1)
        open_lead(2 * pair + 2, 0)
        push(0, 2 * pair + 1).start()
        return carry

    lax.fori_loop(0, count // 2 - 1, ahead, 0)
    open_trail(count - 2, 0)
    open_lead(count - 1, 1)
    open_trail(count - 1, 1)
    push(0, count - 2).start()
    push(0, count - 1).start()

    own = own_ref[...]
    table_v[:nodes, :] = own
    gathered = gath_v[...]
    pre = dot(own, wn_in_ref[:d, :]) + dot(gathered, wn_in_ref[d:, :]) + b_node_ref[...]
    hidden, slope = silu_parts(pre)
    hidden = hidden.astype(BF16)
    y = dot(hidden, wn_out_ref[...])
    y = y - row_mean(y)
    rstd = lax.rsqrt(row_mean(y * y) + 1e-05)
    norm = y * rstd
    node_new_ref[...] = (own.astype(F32) + norm * g_node_ref[...]).astype(BF16)
    node_cot = node_cot_v[...].astype(F32)
    a = node_cot * g_node_ref[...]
    dy = ((a - row_mean(a) - norm * row_mean(a * norm)) * rstd).astype(BF16)
    dpre = (dot(dy, wn_out_ref[...], 1, 1) * slope).astype(BF16)
    dgath_v[...] = dot(dpre, wn_in_ref[d:, :], 1, 1)
    partial_ref[...] = node_cot + dot(dpre, wn_in_ref[:d, :], 1, 1)
    wg_ref[4 * d : 5 * d, :] = dot(own, dpre, 0, 0).astype(BF16)
    wg_ref[5 * d : 6 * d, :] = dot(gathered, dpre, 0, 0).astype(BF16)
    wg_ref[6 * d : 7 * d, :] = dot(hidden, dy, 0, 0).astype(BF16)

    t_acc[...] = jnp.zeros_like(t_acc)
    we_acc[...] = jnp.zeros_like(we_acc)
    wo_acc[...] = jnp.zeros_like(wo_acc)
    lines = lax.broadcasted_iota(jnp.int32, (table, chunk), 0)

    def lead(index, side):
        rows = piece(index)
        cot = cot_v[rows, :].astype(F32)
        buffer = wides[side]
        buffer.spread(dgath_v[part(index), :])
        a = (cot + buffer.get()) * gain
        norm = norm_v[rows, :].astype(F32)
        dy = ((a - row_mean(a) - norm * row_mean(a * norm)) * doubled(scale_v[rows, :])).astype(BF16)
        dpre = dot(dy, back_v[...], 1, 1) * slope_v[rows, :].astype(F32)
        buffer.put(dpre)
        drecv_v[part(index), :] = buffer.folded().astype(BF16)
        dy_v[side] = dy
        dpre_v[side] = dpre.astype(BF16)

    def trail(index, side):
        rows = piece(index)
        dy, dpre = dy_v[side], dpre_v[side]
        grad_v[rows, :] = (cot_v[rows, :].astype(F32) + dot(dpre, w_in_ref[:d, :], 1, 1)).astype(BF16)
        wo_acc[...] += dot(hid_v[rows, :], dy, 0, 0)
        we_acc[...] += dot(edge_v[rows, :], dpre, 0, 0)
        pick = jnp.where(slot_row_ref[:, rows] == lines, 1.0, 0.0).astype(BF16)
        t_acc[...] += dot(pick, dpre)

    for index in range(count):
        pull(index).wait()
    lead(0, 0)

    def behind(pair, carry):
        trail(2 * pair, 0)
        lead(2 * pair + 1, 1)
        push(1, 2 * pair).start()
        trail(2 * pair + 1, 1)
        lead(2 * pair + 2, 0)
        push(1, 2 * pair + 1).start()
        return carry

    lax.fori_loop(0, count // 2 - 1, behind, 0)
    trail(count - 2, 0)
    lead(count - 1, 1)
    trail(count - 1, 1)
    push(1, count - 2).start()
    push(1, count - 1).start()

    total = t_acc[...].astype(BF16)
    for members, ref in ((AHEAD, ahead_back_ref), (BEHIND, behind_back_ref), (SAME, same_back_ref)):
        for place, course in enumerate(members):
            at = nodes + course * cap
            ref[place * cap : (place + 1) * cap, :] = total[at : at + cap, :]
    drecv = drecv_v[...]
    partial_ref[...] += dot(total[:nodes, :], w_in_ref[d : 2 * d, :], 1, 1) + dot(drecv, w_in_ref[2 * d :, :], 1, 1)
    wg_ref[:d, :] = we_acc[...].astype(BF16)
    wg_ref[d : 2 * d, :] = dot(table_v[...], total, 0, 0).astype(BF16)
    wg_ref[2 * d : 3 * d, :] = dot(own, drecv, 0, 0).astype(BF16)
    wg_ref[3 * d : 4 * d, :] = wo_acc[...].astype(BF16)
    for kind in range(2):
        for index in range(count):
            push(kind, index).wait()


def local(
    node_latent,
    edge_latent,
    sender_slot,
    edge_mask,
    send_rows,
    w_edge_in,
    b_edge,
    w_edge_out,
    g_edge,
    w_node_in,
    b_node,
    w_node_out,
    g_node,
    node_cot,
    edge_cot,
):
    nodes, d = node_latent.shape
    edges = edge_latent.shape[0]
    slots = sender_slot.shape[1]
    capacity = send_rows.shape[2]
    far = 8 * capacity
    table = nodes + far
    devices = lax.axis_size("band") * lax.axis_size("sector")
    params = pltpu.CompilerParams(vmem_limit_bytes=34 * 1024 * 1024)
    shape = jax.ShapeDtypeStruct
    rows = send_rows.reshape(8, capacity)
    vmem = pl.BlockSpec(memory_space=pltpu.VMEM)
    hbm = pl.BlockSpec(memory_space=pltpu.HBM)
    free = pl.BlockSpec(memory_space=pl.ANY)
    dma = pltpu.SemaphoreType.DMA

    def off_chip(array):
        return pltpu.with_memory_space_constraint(array, pltpu.HBM)

    def on_chip(array):
        return pltpu.with_memory_space_constraint(array, pltpu.VMEM)

    w_shape = w_edge_in.shape
    ahead, behind, same, own, w_in = pl.pallas_call(
        provide_kernel,
        in_specs=[hbm] * 3,
        out_specs=(vmem,) * 5,
        out_shape=tuple(pltpu.VMEM((len(m) * capacity, d), BF16) for m in (AHEAD, BEHIND, SAME))
        + (pltpu.VMEM((nodes, d), BF16), pltpu.VMEM(w_shape, BF16)),
        scratch_shapes=[pltpu.VMEM(rows.shape, rows.dtype), dma((3,))],
        compiler_params=params,
    )(off_chip(rows), off_chip(node_latent), off_chip(w_edge_in))

    def course_of(course, sets):
        for members, block in sets:
            if course in members:
                at = members.index(course) * capacity
                return block[at : at + capacity]

    def gathered_rows(courses, sets):
        return jnp.concatenate([course_of(course, sets) for course in courses])

    ahead, behind = shifted(ahead, "sector", -1), shifted(behind, "sector", 1)
    sets = ((AHEAD, ahead), (BEHIND, behind), (SAME, same))
    up = shifted(gathered_rows(UP, sets), "band", -1)
    down = shifted(gathered_rows(DOWN, sets), "band", 1)

    chunk = 64 * slots
    count = edges // chunk
    near, code, edge, w_out, wn_in, wn_out, node_cot_near = pl.pallas_call(
        functools.partial(near_kernel, chunk=chunk),
        out_shape=(pltpu.VMEM((edges, d), F32), pltpu.VMEM((edges, 128), jnp.int32), pltpu.VMEM((edges, d), BF16))
        + tuple(pltpu.VMEM(x.shape, BF16) for x in (w_edge_out, w_node_in, w_node_out, node_cot)),
        in_specs=[vmem] * 3 + [free] + [vmem] * 2 + [hbm] * 5,
        out_specs=(vmem,) * 7,
        scratch_shapes=[
            pltpu.VMEM((nodes, d), BF16),
            pltpu.VMEM((nodes, d), F32),
            pltpu.VMEM((d // 128, chunk, 128), F32),
            dma((count,)),
            dma((4,)),
        ],
        compiler_params=params,
        cost_estimate=pl.CostEstimate(flops=6 * edges * d * d, transcendentals=0, bytes_accessed=16 * edges * d),
    )(
        sender_slot,
        edge_mask,
        b_edge.reshape(1, d),
        ahead,
        on_chip(own),
        on_chip(w_in),
        off_chip(edge_latent),
        off_chip(w_edge_out),
        off_chip(w_node_in),
        off_chip(w_node_out),
        off_chip(node_cot),
    )
    node_new, edge_new, partial, edge_grad, ahead_back, behind_back, same_back, grads = pl.pallas_call(
        functools.partial(layer_kernel, chunk=chunk),
        out_shape=(
            shape((nodes, d), BF16),
            shape((edges, d), BF16),
            pltpu.VMEM((nodes, d), F32),
            shape((edges, d), BF16),
            pltpu.VMEM((3 * capacity, d), BF16),
            pltpu.VMEM((3 * capacity, d), BF16),
            pltpu.VMEM((2 * capacity, d), BF16),
            pltpu.VMEM((7 * d, d), BF16),
        ),
        in_specs=[vmem] * 17 + [hbm],
        out_specs=(vmem, hbm, vmem, hbm, vmem, vmem, vmem, vmem),
        scratch_shapes=[
            pltpu.VMEM((edges, d), BF16),
            pltpu.VMEM((edges, d), BF16),
            pltpu.VMEM((edges, d), BF16),
            pltpu.VMEM((edges, d), BF16),
            pltpu.VMEM((edges, d), BF16),
            pltpu.VMEM((edges, d), BF16),
            pltpu.VMEM((edges, 128), F32),
            pltpu.VMEM((table, d), BF16),
            pltpu.VMEM((far, d), BF16),
            pltpu.VMEM((nodes, d), BF16),
            pltpu.VMEM((nodes, d), F32),
            pltpu.VMEM((nodes, d), BF16),
            pltpu.VMEM((2, d // 128, chunk, 128), F32),
            pltpu.VMEM((table, d), F32),
            pltpu.VMEM((d, d), F32),
            pltpu.VMEM((d, d), F32),
            pltpu.VMEM((d, d), BF16),
            pltpu.VMEM((2, chunk, d), BF16),
            pltpu.VMEM((2, chunk, d), BF16),
            dma((count,)),
            dma((2, count)),
        ],
        compiler_params=params,
    )(
        sender_slot.reshape(1, edges),
        g_edge.reshape(1, d),
        b_node.reshape(1, d),
        g_node.reshape(1, d),
        up,
        down,
        ahead,
        behind,
        on_chip(own),
        on_chip(w_in),
        on_chip(near),
        on_chip(code),
        on_chip(edge),
        on_chip(w_out),
        on_chip(wn_in),
        on_chip(wn_out),
        on_chip(node_cot_near),
        off_chip(edge_cot),
    )

    def return_sectors():
        return shifted(ahead_back, "sector", 1), shifted(behind_back, "sector", -1)

    def return_bands(moved):
        sets = ((AHEAD, moved[0]), (BEHIND, moved[1]), (SAME, same_back))
        down, up = over_bands(gathered_rows(DOWN, sets), gathered_rows(UP, sets))
        return up, down, gathered_rows(LEVEL, sets)

    held, got, (up, down, level) = summed_halves(grads, return_sectors, return_bands)
    whole = lambda *dims: pl.BlockSpec(dims, lambda i: (0,) * len(dims))
    node_grad = pl.pallas_call(
        collect_kernel,
        grid=(1,),
        in_specs=[
            whole(8, capacity),
            whole(3 * capacity, d),
            whole(3 * capacity, d),
            whole(2 * capacity, d),
            whole(nodes, d),
            pl.BlockSpec((d, d), lambda i: (1, 0)),
        ],
        out_specs=whole(nodes, d),
        out_shape=shape((nodes, d), F32),
        compiler_params=params,
    )(rows, up, down, level, partial, w_in)
    grad_in, grad_out, grad_node_in, grad_node_out = pl.pallas_call(
        functools.partial(finish_kernel, scale=float(devices * edges) ** (-0.5)),
        in_specs=[pl.BlockSpec(memory_space=pltpu.SMEM), vmem, vmem],
        out_specs=(vmem,) * 4,
        out_shape=tuple(shape((parts * d, d), F32) for parts in (3, 1, 2, 1)),
        compiler_params=params,
    )((position() % 2).reshape(1), held, got)
    return (node_new, edge_new, node_grad, edge_grad, grad_in, grad_out, grad_node_in, grad_node_out)


def solution(mesh):
    split = P(("band", "sector"), None)
    in_specs = (split, split, split, split, P(("band", "sector"), None, None))
    in_specs += (P(),) * 8 + (split, split)
    out_specs = (split,) * 4 + (P(),) * 4
    return jax.shard_map(local, mesh=mesh, in_specs=in_specs, out_specs=out_specs, check_vma=False)
```

```python
import functools

import jax
import jax.numpy as jnp
from jax import lax
from jax.experimental import pallas as pl
from jax.experimental.pallas import tpu as pltpu
from jax.sharding import PartitionSpec as P

band_steps = (-1, -1, -1, 0, 0, 1, 1, 1)
sector_steps = (-1, 0, 1, -1, 1, -1, 0, 1)
AHEAD = tuple(j for j in range(8) if sector_steps[j] == 1)
BEHIND = tuple(j for j in range(8) if sector_steps[j] == -1)
SAME = tuple(j for j in range(8) if sector_steps[j] == 0)
UP = tuple(j for j in range(8) if band_steps[j] == 1)
DOWN = tuple(j for j in range(8) if band_steps[j] == -1)
LEVEL = tuple(j for j in range(8) if band_steps[j] == 0)
BF16 = jnp.bfloat16
F32 = jnp.float32


def shifted(array, axis, by):
    count = lax.axis_size(axis)
    return lax.ppermute(array, axis, [(i, (i + by) % count) for i in range(count)])


def over_bands(up, down):
    count = lax.axis_size("band")
    if count % 2:
        return shifted(up, "band", -1), shifted(down, "band", 1)
    even = lax.axis_index("band") % 2 == 0
    near = [(i, i ^ 1) for i in range(count)]
    cross = [(i, i if i in (0, count - 1) else i + 1 if i % 2 else i - 1) for i in range(count)]
    first = lax.ppermute(jnp.where(even, down, up), "band", near)
    second = lax.ppermute(jnp.where(even, up, down), "band", cross)
    return jnp.where(even, first, second), jnp.where(even, second, first)


def flipped(array, mask):
    count = lax.axis_size("band") * lax.axis_size("sector")
    return lax.ppermute(array, ("band", "sector"), [(i, i ^ mask) for i in range(count)])


def position():
    return lax.axis_index("band") * lax.axis_size("sector") + lax.axis_index("sector")


def quarter(array, index):
    rows = array.shape[0] // 4
    return lax.dynamic_slice_in_dim(array, index * rows, rows, 0)


def plus(first, *others):
    total = first.astype(F32)
    for other in others:
        total = total + other.astype(F32)
    return total.astype(BF16)


def summed_halves(array, beside_first, beside_second):
    count = lax.axis_size("band") * lax.axis_size("sector")
    here = position()
    half = array.shape[0] // 2
    bit = here % 2
    give = lax.dynamic_slice_in_dim(array, (1 - bit) * half, half, 0)
    keep = lax.dynamic_slice_in_dim(array, bit * half, half, 0)
    held = plus(keep, flipped(give, 1))
    place = (here // 2) % 4
    got = [flipped(quarter(held, place ^ turn), 2 * turn) for turn in (3, 1, 2)]
    part = plus(quarter(held, place), *got)
    part, first = lax.optimization_barrier((part, beside_first()))
    second = beside_second(first)
    masks, step = [], 8
    while step < count:
        masks.append(step)
        step *= 2
    if len(masks) > 1:
        masks[1] |= masks[0]
    for mask in masks:
        part = plus(part, flipped(part, mask))
    parts = {turn: flipped(part, 2 * turn) for turn in (3, 1, 2)}
    parts[0] = part
    rows = []
    for at in range(4):
        chosen = parts[at ^ 3]
        for turn in range(3):
            chosen = jnp.where(place == turn, parts[at ^ turn], chosen)
        rows.append(chosen)
    held, second = lax.optimization_barrier((jnp.concatenate(rows), second))
    return held, flipped(held, 1), second


def dot(a, b, ca=1, cb=0):
    return lax.dot_general(a, b, (((ca,), (cb,)), ((), ())), preferred_element_type=F32)


def doubled(values):
    return jnp.concatenate([values, values], axis=1)


def row_mean(values):
    return jnp.mean(values, axis=-1, keepdims=True)


def silu_parts(v):
    gate = 0.5 * jnp.tanh(0.5 * v) + 0.5
    out = v * gate
    return out, gate + out * (1.0 - gate)


def picked(rows, count):
    flat = jnp.concatenate([rows[j : j + 1, :] for j in range(rows.shape[0])], axis=1)
    lines = lax.broadcasted_iota(jnp.int32, (count, flat.shape[1]), 0)
    return jnp.where(flat == lines, 1.0, 0.0).astype(BF16)


def provide_kernel(rows_hbm, node_hbm, w_hbm, ahead_ref, behind_ref, same_ref, own_ref, w_ref, rows_ref, sem):
    copies = [
        pltpu.make_async_copy(src, dst, sem.at[place])
        for place, (src, dst) in enumerate(
            ((rows_hbm, rows_ref), (node_hbm, own_ref), (w_hbm, w_ref))
        )
    ]
    for copy in copies:
        copy.start()
    copies[0].wait()
    pick = picked(rows_ref[...], own_ref.shape[0])
    copies[1].wait()
    rows = dot(pick, own_ref[...], 0, 0).astype(BF16)
    cap = rows_ref.shape[1]
    for ref, members in ((ahead_ref, AHEAD), (behind_ref, BEHIND), (same_ref, SAME)):
        for place, course in enumerate(members):
            ref[place * cap : (place + 1) * cap, :] = rows[course * cap : (course + 1) * cap, :]
    copies[2].wait()


def collect_kernel(rows_ref, up_ref, down_ref, level_ref, partial_ref, w_ref, out_ref):
    cap = rows_ref.shape[1]
    pieces = {}
    for ref, members in ((up_ref, UP), (down_ref, DOWN), (level_ref, LEVEL)):
        for place, course in enumerate(members):
            pieces[course] = ref[place * cap : (place + 1) * cap, :]
    arrived = jnp.concatenate([pieces[course] for course in range(8)])
    total = dot(picked(rows_ref[...], partial_ref.shape[0]), arrived).astype(BF16)
    out_ref[...] = partial_ref[...] + dot(total, w_ref[...], 1, 1)


def finish_kernel(bit_ref, held_ref, got_ref, in_ref, out_ref, node_in_ref, node_out_ref, *, scale):
    first = bit_ref[0] == 0
    held = held_ref[...].astype(F32) * scale
    got = got_ref[...].astype(F32) * scale
    halves = (jnp.where(first, held, got), jnp.where(first, got, held))
    half = held.shape[0]
    start = 0
    for ref in (in_ref, out_ref, node_in_ref, node_out_ref):
        rows = ref.shape[0]
        for side in range(2):
            lo, hi = max(start, side * half), min(start + rows, (side + 1) * half)
            if lo < hi:
                ref[lo - start : hi - start, :] = halves[side][lo - side * half : hi - side * half, :]
        start += rows


def pieces_of(chunk):
    def piece(index):
        return pl.ds(pl.multiple_of(index * chunk, chunk), chunk)

    return piece


def one_hot(values, lanes, first, last):
    parts = [jnp.where(values == lanes + at, 1.0, 0.0).astype(BF16) for at in range(first, last, 128)]
    return jnp.concatenate(parts, axis=1)


class Wide:
    def __init__(self, ref, slots):
        self.ref, self.slots = ref, slots
        self.blocks, self.rows = ref.shape[0], ref.shape[1] // slots

    def spread(self, rows):
        for k in range(self.slots):
            for block in range(self.blocks):
                part = rows[:, block * 128 : (block + 1) * 128]
                self.ref[block, pl.ds(k, self.rows, stride=self.slots), :] = part

    def get(self):
        return jnp.concatenate([self.ref[block] for block in range(self.blocks)], axis=1)

    def put(self, values):
        for block in range(self.blocks):
            self.ref[block] = values[:, block * 128 : (block + 1) * 128]

    def folded(self):
        parts = []
        for block in range(self.blocks):
            total = self.ref[block, pl.ds(0, self.rows, stride=self.slots), :]
            for k in range(1, self.slots):
                total = total + self.ref[block, pl.ds(k, self.rows, stride=self.slots), :]
            parts.append(total)
        return jnp.concatenate(parts, axis=1)


def near_kernel(
    slot_ref,
    mask_ref,
    b_edge_hbm,
    after_ref,
    own_ref,
    w_in_ref,
    edge_hbm,
    w_out_hbm,
    wn_in_hbm,
    wn_out_hbm,
    node_cot_hbm,
    near_ref,
    code_ref,
    edge_ref,
    w_out_ref,
    wn_in_ref,
    wn_out_ref,
    node_cot_ref,
    proj_v,
    recv_v,
    wide_v,
    b_edge_v,
    sem_in,
    sem_whole,
    *,
    chunk,
):
    nodes, d = own_ref.shape
    edges = edge_ref.shape[0]
    slots = edges // nodes
    count = edges // chunk
    cn = chunk // slots
    piece = pieces_of(chunk)

    def pull(index):
        return pltpu.make_async_copy(edge_hbm.at[piece(index)], edge_ref.at[piece(index)], sem_in.at[index])

    wholes = [
        pltpu.make_async_copy(src, dst, sem_whole.at[place])
        for place, (src, dst) in enumerate(
            (
                (w_out_hbm, w_out_ref),
                (wn_in_hbm, wn_in_ref),
                (wn_out_hbm, wn_out_ref),
                (node_cot_hbm, node_cot_ref),
                (b_edge_hbm, b_edge_v),
            )
        )
    ]
    wholes[-1].start()
    for index in range(count):
        pull(index).start()
    for copy in wholes[:-1]:
        copy.start()
    code = slot_ref[...] * 2 + mask_ref[...]
    for k in range(slots):
        code_ref[pl.ds(k, nodes, stride=slots), :] = jnp.broadcast_to(code[:, k : k + 1], (nodes, 128))
    own = own_ref[...]
    proj_v[...] = dot(own, w_in_ref[d : 2 * d, :]).astype(BF16)
    wholes[-1].wait()
    recv_v[...] = dot(own, w_in_ref[2 * d :, :]) + b_edge_v[...]
    lanes = lax.broadcasted_iota(jnp.int32, (chunk, 128), 1)
    wide = Wide(wide_v, slots)

    def step(index, carry):
        rows = piece(index)
        pull(index).wait()
        wide.spread(recv_v[pl.ds(pl.multiple_of(index * cn, cn), cn), :])
        pick = one_hot(lax.shift_right_logical(code_ref[rows, :], 1), lanes, 0, nodes)
        near_ref[rows, :] = 0.5 * (dot(edge_ref[rows, :], w_in_ref[:d, :]) + dot(pick, proj_v[...]) + wide.get())
        return carry

    lax.fori_loop(0, count, step, 0)
    for copy in wholes[:-1]:
        copy.wait()


def layer_kernel(
    slot_row_ref,
    g_edge_ref,
    b_node_ref,
    g_node_ref,
    up_ref,
    down_ref,
    ahead_ref,
    behind_ref,
    own_ref,
    w_in_ref,
    near_v,
    code_v,
    edge_v,
    w_out_ref,
    wn_in_ref,
    wn_out_ref,
    node_cot_v,
    cot_hbm,
    node_new_ref,
    new_hbm,
    partial_ref,
    grad_hbm,
    ahead_back_ref,
    behind_back_ref,
    same_back_ref,
    wg_ref,
    cot_v,
    new_v,
    grad_v,
    hid_v,
    slope_v,
    norm_v,
    scale_v,
    table_v,
    proj_v,
    gath_v,
    dgath_v,
    drecv_v,
    wide_v,
    t_acc,
    we_acc,
    wo_acc,
    back_v,
    dy_v,
    dpre_v,
    sem_in,
    sem_out,
    *,
    chunk,
):
    nodes, d = own_ref.shape
    edges = edge_v.shape[0]
    slots = edges // nodes
    cap = up_ref.shape[0] // 3
    table = nodes + 8 * cap
    count = edges // chunk
    cn = chunk // slots
    piece = pieces_of(chunk)

    def pull(index):
        return pltpu.make_async_copy(cot_hbm.at[piece(index)], cot_v.at[piece(index)], sem_in.at[index])

    def push(kind, index):
        src, dst = ((new_v, new_hbm), (grad_v, grad_hbm))[kind]
        return pltpu.make_async_copy(src.at[piece(index)], dst.at[piece(index)], sem_out.at[kind, index])

    for index in range(count):
        pull(index).start()

    level = (behind_ref[cap : 2 * cap, :], ahead_ref[cap : 2 * cap, :])
    for members, rows in ((UP, up_ref[...]), (DOWN, down_ref[...]), (LEVEL, jnp.concatenate(level))):
        for place, course in enumerate(members):
            at = nodes + course * cap
            table_v[at : at + cap, :] = rows[place * cap : (place + 1) * cap, :]
    proj_v[...] = (0.5 * dot(table_v[nodes:, :], w_in_ref[d : 2 * d, :])).astype(BF16)
    back_v[...] = 0.5 * w_out_ref[...]
    gain = g_edge_ref[...]
    lanes = lax.broadcasted_iota(jnp.int32, (chunk, 128), 1)
    wides = (Wide(wide_v.at[0], slots), Wide(wide_v.at[1], slots))
    wide = wides[0]

    def part(index):
        return pl.ds(pl.multiple_of(index * cn, cn), cn)

    def open_lead(index, side):
        rows = piece(index)
        pick = one_hot(lax.shift_right_logical(code_v[rows, :], 1), lanes, nodes, table)
        half = near_v[rows, :] + dot(pick, proj_v[...])
        bend = jnp.tanh(half)
        gate = bend + 1.0
        hidden = half * gate
        slope_v[rows, :] = (gate + hidden * (1.0 - bend)).astype(BF16)
        hidden = hidden.astype(BF16)
        hid_v[rows, :] = hidden
        dy_v[side] = hidden

    def open_trail(index, side):
        rows = piece(index)
        buffer = wides[side]
        y = dot(dy_v[side], w_out_ref[...])
        y = y - row_mean(y)
        rstd = lax.rsqrt(row_mean(y * y) + 1e-05)
        scale = (code_v[rows, :] & 1).astype(F32) * rstd
        scale_v[rows, :] = scale
        norm = y * doubled(scale)
        norm_v[rows, :] = norm.astype(BF16)
        update = norm * gain
        new_v[rows, :] = (edge_v[rows, :].astype(F32) + update).astype(BF16)
        buffer.put(update)
        gath_v[part(index), :] = buffer.folded().astype(BF16)

    open_lead(0, 0)

    def ahead(pair, carry):
        open_trail(2 * pair, 0)
        open_lead(2 * pair + 1, 1)
        push(0, 2 * pair).start()
        open_trail(2 * pair + 1, 1)
        open_lead(2 * pair + 2, 0)
        push(0, 2 * pair + 1).start()
        return carry

    lax.fori_loop(0, count // 2 - 1, ahead, 0)
    open_trail(count - 2, 0)
    open_lead(count - 1, 1)
    open_trail(count - 1, 1)
    push(0, count - 2).start()
    push(0, count - 1).start()

    own = own_ref[...]
    table_v[:nodes, :] = own
    gathered = gath_v[...]
    pre = dot(own, wn_in_ref[:d, :]) + dot(gathered, wn_in_ref[d:, :]) + b_node_ref[...]
    hidden, slope = silu_parts(pre)
    hidden = hidden.astype(BF16)
    y = dot(hidden, wn_out_ref[...])
    y = y - row_mean(y)
    rstd = lax.rsqrt(row_mean(y * y) + 1e-05)
    norm = y * rstd
    node_new_ref[...] = (own.astype(F32) + norm * g_node_ref[...]).astype(BF16)
    node_cot = node_cot_v[...].astype(F32)
    a = node_cot * g_node_ref[...]
    dy = ((a - row_mean(a) - norm * row_mean(a * norm)) * rstd).astype(BF16)
    dpre = (dot(dy, wn_out_ref[...], 1, 1) * slope).astype(BF16)
    dgath_v[...] = dot(dpre, wn_in_ref[d:, :], 1, 1)
    partial_ref[...] = node_cot + dot(dpre, wn_in_ref[:d, :], 1, 1)
    wg_ref[4 * d : 5 * d, :] = dot(own, dpre, 0, 0).astype(BF16)
    wg_ref[5 * d : 6 * d, :] = dot(gathered, dpre, 0, 0).astype(BF16)
    wg_ref[6 * d : 7 * d, :] = dot(hidden, dy, 0, 0).astype(BF16)

    t_acc[...] = jnp.zeros_like(t_acc)
    we_acc[...] = jnp.zeros_like(we_acc)
    wo_acc[...] = jnp.zeros_like(wo_acc)
    lines = lax.broadcasted_iota(jnp.int32, (table, chunk), 0)

    def lead(index, side):
        rows = piece(index)
        cot = cot_v[rows, :].astype(F32)
        buffer = wides[side]
        buffer.spread(dgath_v[part(index), :])
        a = (cot + buffer.get()) * gain
        norm = norm_v[rows, :].astype(F32)
        dy = ((a - row_mean(a) - norm * row_mean(a * norm)) * doubled(scale_v[rows, :])).astype(BF16)
        dpre = dot(dy, back_v[...], 1, 1) * slope_v[rows, :].astype(F32)
        buffer.put(dpre)
        drecv_v[part(index), :] = buffer.folded().astype(BF16)
        dy_v[side] = dy
        dpre_v[side] = dpre.astype(BF16)

    def trail(index, side):
        rows = piece(index)
        dy, dpre = dy_v[side], dpre_v[side]
        grad_v[rows, :] = (cot_v[rows, :].astype(F32) + dot(dpre, w_in_ref[:d, :], 1, 1)).astype(BF16)
        wo_acc[...] += dot(hid_v[rows, :], dy, 0, 0)
        we_acc[...] += dot(edge_v[rows, :], dpre, 0, 0)
        pick = jnp.where(slot_row_ref[:, rows] == lines, 1.0, 0.0).astype(BF16)
        t_acc[...] += dot(pick, dpre)

    for index in range(count):
        pull(index).wait()
    lead(0, 0)

    def behind(pair, carry):
        trail(2 * pair, 0)
        lead(2 * pair + 1, 1)
        push(1, 2 * pair).start()
        trail(2 * pair + 1, 1)
        lead(2 * pair + 2, 0)
        push(1, 2 * pair + 1).start()
        return carry

    lax.fori_loop(0, count // 2 - 1, behind, 0)
    trail(count - 2, 0)
    lead(count - 1, 1)
    trail(count - 1, 1)
    push(1, count - 2).start()
    push(1, count - 1).start()

    total = t_acc[...].astype(BF16)
    for members, ref in ((AHEAD, ahead_back_ref), (BEHIND, behind_back_ref), (SAME, same_back_ref)):
        for place, course in enumerate(members):
            at = nodes + course * cap
            ref[place * cap : (place + 1) * cap, :] = total[at : at + cap, :]
    drecv = drecv_v[...]
    partial_ref[...] += dot(total[:nodes, :], w_in_ref[d : 2 * d, :], 1, 1) + dot(drecv, w_in_ref[2 * d :, :], 1, 1)
    wg_ref[:d, :] = we_acc[...].astype(BF16)
    wg_ref[d : 2 * d, :] = dot(table_v[...], total, 0, 0).astype(BF16)
    wg_ref[2 * d : 3 * d, :] = dot(own, drecv, 0, 0).astype(BF16)
    wg_ref[3 * d : 4 * d, :] = wo_acc[...].astype(BF16)
    for kind in range(2):
        for index in range(count):
            push(kind, index).wait()


def local(
    node_latent,
    edge_latent,
    sender_slot,
    edge_mask,
    send_rows,
    w_edge_in,
    b_edge,
    w_edge_out,
    g_edge,
    w_node_in,
    b_node,
    w_node_out,
    g_node,
    node_cot,
    edge_cot,
):
    nodes, d = node_latent.shape
    edges = edge_latent.shape[0]
    slots = sender_slot.shape[1]
    capacity = send_rows.shape[2]
    far = 8 * capacity
    table = nodes + far
    devices = lax.axis_size("band") * lax.axis_size("sector")
    params = pltpu.CompilerParams(vmem_limit_bytes=34 * 1024 * 1024)
    shape = jax.ShapeDtypeStruct
    rows = send_rows.reshape(8, capacity)
    vmem = pl.BlockSpec(memory_space=pltpu.VMEM)
    hbm = pl.BlockSpec(memory_space=pltpu.HBM)
    free = pl.BlockSpec(memory_space=pl.ANY)
    dma = pltpu.SemaphoreType.DMA

    def off_chip(array):
        return pltpu.with_memory_space_constraint(array, pltpu.HBM)

    def on_chip(array):
        return pltpu.with_memory_space_constraint(array, pltpu.VMEM)

    w_shape = w_edge_in.shape
    ahead, behind, same, own, w_in = pl.pallas_call(
        provide_kernel,
        in_specs=[hbm] * 3,
        out_specs=(vmem,) * 5,
        out_shape=tuple(pltpu.VMEM((len(m) * capacity, d), BF16) for m in (AHEAD, BEHIND, SAME))
        + (pltpu.VMEM((nodes, d), BF16), pltpu.VMEM(w_shape, BF16)),
        scratch_shapes=[pltpu.VMEM(rows.shape, rows.dtype), dma((3,))],
        compiler_params=params,
    )(off_chip(rows), off_chip(node_latent), off_chip(w_edge_in))

    def course_of(course, sets):
        for members, block in sets:
            if course in members:
                at = members.index(course) * capacity
                return block[at : at + capacity]

    def gathered_rows(courses, sets):
        return jnp.concatenate([course_of(course, sets) for course in courses])

    ahead, behind = shifted(ahead, "sector", -1), shifted(behind, "sector", 1)
    sets = ((AHEAD, ahead), (BEHIND, behind), (SAME, same))
    up = shifted(gathered_rows(UP, sets), "band", -1)
    down = shifted(gathered_rows(DOWN, sets), "band", 1)

    chunk = 64 * slots
    count = edges // chunk
    near, code, edge, w_out, wn_in, wn_out, node_cot_near = pl.pallas_call(
        functools.partial(near_kernel, chunk=chunk),
        out_shape=(pltpu.VMEM((edges, d), F32), pltpu.VMEM((edges, 128), jnp.int32), pltpu.VMEM((edges, d), BF16))
        + tuple(pltpu.VMEM(x.shape, BF16) for x in (w_edge_out, w_node_in, w_node_out, node_cot)),
        in_specs=[vmem] * 2 + [hbm, free] + [vmem] * 2 + [hbm] * 5,
        out_specs=(vmem,) * 7,
        scratch_shapes=[
            pltpu.VMEM((nodes, d), BF16),
            pltpu.VMEM((nodes, d), F32),
            pltpu.VMEM((d // 128, chunk, 128), F32),
            pltpu.VMEM((1, d), F32),
            dma((count,)),
            dma((5,)),
        ],
        compiler_params=params,
        cost_estimate=pl.CostEstimate(flops=6 * edges * d * d, transcendentals=0, bytes_accessed=16 * edges * d),
    )(
        sender_slot,
        edge_mask,
        off_chip(b_edge.reshape(1, d)),
        ahead,
        on_chip(own),
        on_chip(w_in),
        off_chip(edge_latent),
        off_chip(w_edge_out),
        off_chip(w_node_in),
        off_chip(w_node_out),
        off_chip(node_cot),
    )
    node_new, edge_new, partial, edge_grad, ahead_back, behind_back, same_back, grads = pl.pallas_call(
        functools.partial(layer_kernel, chunk=chunk),
        out_shape=(
            shape((nodes, d), BF16),
            shape((edges, d), BF16),
            pltpu.VMEM((nodes, d), F32),
            shape((edges, d), BF16),
            pltpu.VMEM((3 * capacity, d), BF16),
            pltpu.VMEM((3 * capacity, d), BF16),
            pltpu.VMEM((2 * capacity, d), BF16),
            pltpu.VMEM((7 * d, d), BF16),
        ),
        in_specs=[vmem] * 17 + [hbm],
        out_specs=(vmem, hbm, vmem, hbm, vmem, vmem, vmem, vmem),
        scratch_shapes=[
            pltpu.VMEM((edges, d), BF16),
            pltpu.VMEM((edges, d), BF16),
            pltpu.VMEM((edges, d), BF16),
            pltpu.VMEM((edges, d), BF16),
            pltpu.VMEM((edges, d), BF16),
            pltpu.VMEM((edges, d), BF16),
            pltpu.VMEM((edges, 128), F32),
            pltpu.VMEM((table, d), BF16),
            pltpu.VMEM((far, d), BF16),
            pltpu.VMEM((nodes, d), BF16),
            pltpu.VMEM((nodes, d), F32),
            pltpu.VMEM((nodes, d), BF16),
            pltpu.VMEM((2, d // 128, chunk, 128), F32),
            pltpu.VMEM((table, d), F32),
            pltpu.VMEM((d, d), F32),
            pltpu.VMEM((d, d), F32),
            pltpu.VMEM((d, d), BF16),
            pltpu.VMEM((2, chunk, d), BF16),
            pltpu.VMEM((2, chunk, d), BF16),
            dma((count,)),
            dma((2, count)),
        ],
        compiler_params=params,
    )(
        sender_slot.reshape(1, edges),
        g_edge.reshape(1, d),
        b_node.reshape(1, d),
        g_node.reshape(1, d),
        up,
        down,
        ahead,
        behind,
        on_chip(own),
        on_chip(w_in),
        on_chip(near),
        on_chip(code),
        on_chip(edge),
        on_chip(w_out),
        on_chip(wn_in),
        on_chip(wn_out),
        on_chip(node_cot_near),
        off_chip(edge_cot),
    )

    def return_sectors():
        return shifted(ahead_back, "sector", 1), shifted(behind_back, "sector", -1)

    def return_bands(moved):
        sets = ((AHEAD, moved[0]), (BEHIND, moved[1]), (SAME, same_back))
        down, up = over_bands(gathered_rows(DOWN, sets), gathered_rows(UP, sets))
        return up, down, gathered_rows(LEVEL, sets)

    held, got, (up, down, level) = summed_halves(grads, return_sectors, return_bands)
    whole = lambda *dims: pl.BlockSpec(dims, lambda i: (0,) * len(dims))
    node_grad = pl.pallas_call(
        collect_kernel,
        grid=(1,),
        in_specs=[
            whole(8, capacity),
            whole(3 * capacity, d),
            whole(3 * capacity, d),
            whole(2 * capacity, d),
            whole(nodes, d),
            pl.BlockSpec((d, d), lambda i: (1, 0)),
        ],
        out_specs=whole(nodes, d),
        out_shape=shape((nodes, d), F32),
        compiler_params=params,
    )(rows, up, down, level, partial, w_in)
    grad_in, grad_out, grad_node_in, grad_node_out = pl.pallas_call(
        functools.partial(finish_kernel, scale=float(devices * edges) ** (-0.5)),
        in_specs=[pl.BlockSpec(memory_space=pltpu.SMEM), vmem, vmem],
        out_specs=(vmem,) * 4,
        out_shape=tuple(shape((parts * d, d), F32) for parts in (3, 1, 2, 1)),
        compiler_params=params,
    )((position() % 2).reshape(1), held, got)
    return (node_new, edge_new, node_grad, edge_grad, grad_in, grad_out, grad_node_in, grad_node_out)


def solution(mesh):
    split = P(("band", "sector"), None)
    in_specs = (split, split, split, split, P(("band", "sector"), None, None))
    in_specs += (P(),) * 8 + (split, split)
    out_specs = (split,) * 4 + (P(),) * 4
    return jax.shard_map(local, mesh=mesh, in_specs=in_specs, out_specs=out_specs, check_vma=False)
```
